128 devices in a mesh: dp: 2 (over z_hi), expert: 64 (over z_lo, y, x, core).
Axes of the slice: x: 4, y: 4, z: 4 (z_hi: 2, z_lo: 2; z = z_hi * 2 + z_lo), core: 2. Of those that a mesh axis runs over, the one named last changes fastest.
Arguments:
- tokens_in: bfloat16 [16384, 2880], P(('dp', 'expert')), may hold values from -6 to 6
- grad_out: bfloat16 [16384, 2880], P(('dp', 'expert')), may hold values from -6 to 6
- expert_ids: int32 [16384, 4], P(('dp', 'expert')), may hold values from 0 to 63, all different within a row; in each aligned block of 128 rows (0 to 127, 128 to 255, ...) at most 10 rows name the same one
- combine_weights: float32 [16384, 4], P(('dp', 'expert')), may hold values from 0.1 to 1
- up_weight: bfloat16 [64, 2880, 1440], P('expert'), may hold values from -0.109375 to 0.109375
- down_weight: bfloat16 [64, 1440, 2880], P('expert'), may hold values from -0.15625 to 0.15625
Outputs:
- grad_input: bfloat16 [16384, 2880], P(('dp', 'expert'))
- grad_up: bfloat16 [64, 2880, 1440], P('expert', 'dp')
- grad_down: bfloat16 [64, 1440, 2880], P('expert', 'dp')
The draws below stay inside these ranges and needn't reach their ends.
Inputs may be any that keep to these rules, and one draw needn't show every extreme that they name: `expert_ids`: each row names 4 different experts; in the rows of one device no expert is named by more than 10 rows, a bound that some block reaches.
All inputs are finite; a program needn't handle non-finite values.
Results may differ from the reference program's by a relative error of at most 0.0064.
Values may be sent and summed in bfloat16 or wider, within the bound.
No kernel may reach another device: no remote copies, remote signals or barrier semaphores. Data moves between devices by JAX's collectives and lax.ppermute only.
A program may use at most 192 MiB of HBM per device.

```python
import math
import jax
import jax.numpy as jnp
import numpy as np
from jax import lax

D = 2880
F = 1440
TOPK = 4
TOK_DEV = 128
EXPERTS = 64
CAP = 10
TOKENS = 16384
N_DP = 2
N_EXPERT = 64


def level_of(key, dims, pieces, smallest, top_value):
    factor_of, own = 1.0, jax.random.fold_in(key, 6)
    for dim, blocks in pieces:
        steps = jnp.exp(jax.random.uniform(jax.random.fold_in(own, dim), (blocks,), jnp.float32, smallest / len(pieces), top_value / len(pieces)))
        factor_of = factor_of * jnp.repeat(steps, dims[dim] // blocks).reshape([-1 if axis == dim else 1 for axis in range(len(dims))])
    return factor_of


def deal_out(rng, own, number, rows, amount, top, reach, skew):
    ranking = jax.random.permutation(rng, amount)
    crowded, ordinary = portions_of(amount, rows * top, reach, skew, True), portions_of(amount, rows * top, reach, skew, False)
    places = jnp.arange(amount)

    def named(tallies, turn):
        used = int((tallies > 0).sum())
        fixed = max(1, used // 4)
        passed = fixed + (places - fixed + turn * (used - fixed)) % max(1, amount - fixed)
        return jnp.zeros((amount,), jnp.int32).at[ranking[jnp.where(places < fixed, places, passed)]].set(jnp.asarray(tallies, jnp.int32))

    tallies = jnp.where(number % 4 == 0, named(crowded, number // 4), named(ordinary, number - number // 4 - 1))
    mixed = jax.random.permutation(jax.random.fold_in(own, 3), amount)
    source_of, taker = mixed[0:amount // 2 * 2:2], mixed[1:amount // 2 * 2:2]
    margin = jnp.minimum(tallies[source_of] - 1, reach - tallies[taker]) // 2
    margin = jnp.where((source_of == ranking[0]) | (taker == ranking[0]) | (tallies[taker] == 0), 0, jnp.maximum(margin, 0))
    passed = jax.random.randint(jax.random.fold_in(own, 4), (amount // 2,), 0, 1 << 20) % (margin + 1)
    tallies = tallies.at[source_of].add(-passed).at[taker].add(passed)
    labels = jnp.searchsorted(jnp.cumsum(tallies), jnp.arange(rows * top), side="right").astype(jnp.int32)
    table = labels.reshape(top, rows).T
    table = table[jax.random.permutation(jax.random.fold_in(own, 1), rows)]
    turn = jax.random.randint(jax.random.fold_in(own, 2), (rows, 1), 0, top)
    return jnp.take_along_axis(table, (jnp.arange(top)[None, :] + turn) % top, axis=1)


def portions_of(amount, total, reach, skew, full):
    portions = [(1 << 20) // math.isqrt(standing ** skew) + 1 for standing in range(1, amount + 1)]
    largest = reach if full else min(reach, max(-(-total // amount), total * portions[0] // sum(portions)))
    least = 1 if total - largest >= amount - 1 else 0
    counts, surplus = [largest] + [least] * (amount - 1), total - largest - least * (amount - 1)
    while surplus > 0:
        movable = [i for i in range(1, amount) if counts[i] < largest] or [i for i in range(1, amount) if counts[i] < reach]
        mass, remaining = sum([portions[i] for i in movable]), surplus
        for i in movable:
            extra = min(reach - counts[i], max(1, remaining * portions[i] // mass), surplus)
            counts[i] = counts[i] + extra
            surplus = surplus - extra
    return np.array(counts)


def bell_draw(own_key, dims, deviation, bound, shards=(), kind=jnp.bfloat16):
    array = jax.random.normal(own_key, dims, jnp.float32) * deviation
    if len(shards) > 0:
        array = level_of(own_key, dims, shards, -0.22, 0.18) * array
    return jnp.clip(array, min=-bound, max=bound).astype(kind)


def setup_inputs(seed: int = 0) -> dict:
    key_list = jax.random.split(jax.random.key(seed), 7)
    tokens_in = bell_draw(key_list[0], (TOKENS, D), 1.0, 6.0, ((0, 128),))
    grad_out = bell_draw(key_list[1], (TOKENS, D), 1.0, 6.0, ((0, 128),))
    expert_ids_keys = jax.random.split(jax.random.fold_in(key_list[2], 1), TOKENS // TOK_DEV)
    expert_ids_turns = jax.random.permutation(jax.random.fold_in(key_list[2], 3), TOKENS // TOK_DEV)
    expert_ids = jax.vmap(lambda own, number: deal_out(jax.random.fold_in(key_list[2], 2), own, number, TOK_DEV, EXPERTS, TOPK, CAP, 1))(expert_ids_keys, expert_ids_turns).reshape((TOKENS, TOPK))
    combine_weights = jnp.clip(jnp.exp(math.log(1.0) - 2.3025851 * jax.random.uniform(key_list[3], (TOKENS, TOPK), jnp.float32) ** level_of(key_list[3], (TOKENS, TOPK), ((0, 128),), -0.2, 0.2)), 0.1, 1.0)
    up_weight = bell_draw(key_list[4], (EXPERTS, D, F), D ** -0.5, 0.109375, ((0, 64),))
    down_weight = bell_draw(key_list[5], (EXPERTS, F, D), F ** -0.5, 0.15625, ((0, 64),))
    return dict(tokens_in=tokens_in, grad_out=grad_out, expert_ids=expert_ids, combine_weights=combine_weights, up_weight=up_weight, down_weight=down_weight)


def silu_parts(preact):
    logistic = jax.nn.sigmoid(preact)
    return preact * logistic, logistic * (1.0 + preact * (1.0 - logistic))


def reference(tokens_in, grad_out, expert_ids, combine_weights, up_weight, down_weight):
    model_width = tokens_in.shape[1]
    devices_all = N_DP * N_EXPERT
    block_rows = TOK_DEV * TOPK
    per_expert = devices_all * CAP
    routed = TOKENS * TOPK
    flat_ids = expert_ids.reshape(devices_all, block_rows)
    one_hot = (flat_ids[:, :, None] == jnp.arange(EXPERTS, dtype=jnp.int32)[None, None, :]).astype(jnp.int32)
    slot_rank = jnp.sum((jnp.cumsum(one_hot, axis=1) - one_hot) * one_hot, axis=2)
    source_dev = jnp.arange(devices_all, dtype=jnp.int32)[:, None]
    position = (flat_ids * per_expert + source_dev * CAP + slot_rank).reshape(-1).astype(jnp.int32)
    slot_table = jnp.full((EXPERTS * per_expert,), routed, jnp.int32).at[position].set(jnp.arange(routed, dtype=jnp.int32))
    padded_x = jnp.concatenate([tokens_in, jnp.zeros((1, model_width), tokens_in.dtype)], axis=0)
    padded_dy = jnp.concatenate([grad_out, jnp.zeros((1, model_width), grad_out.dtype)], axis=0)
    padded_weight = jnp.concatenate([combine_weights.reshape(-1), jnp.zeros((1,), combine_weights.dtype)], axis=0)

    def one_expert(operands):
        rows_idx, w_up, w_down = operands
        source_token = rows_idx // TOPK
        rows_x = padded_x[source_token]
        rows_grad = (padded_weight[rows_idx][:, None] * padded_dy[source_token].astype(jnp.float32)).astype(jnp.bfloat16)
        preact = jnp.dot(rows_x, w_up, preferred_element_type=jnp.float32)
        activated, slope = silu_parts(preact)
        activated = activated.astype(jnp.bfloat16)
        grad_act = jnp.dot(rows_grad, w_down.T, preferred_element_type=jnp.float32)
        grad_pre = (grad_act * slope).astype(jnp.bfloat16)
        grad_rows = jnp.dot(grad_pre, w_up.T, preferred_element_type=jnp.float32).astype(jnp.bfloat16)
        grad_upper = jnp.dot(rows_x.T, grad_pre, preferred_element_type=jnp.float32).astype(jnp.bfloat16)
        grad_lower = jnp.dot(activated.T, rows_grad, preferred_element_type=jnp.float32).astype(jnp.bfloat16)
        return grad_rows, grad_upper, grad_lower

    grad_rows, grad_up, grad_down = lax.map(one_expert, (slot_table.reshape(EXPERTS, per_expert), up_weight, down_weight))
    picked = grad_rows.reshape(-1, model_width)[position].reshape(TOKENS, TOPK, model_width)
    grad_input = jnp.sum(picked.astype(jnp.float32), axis=1).astype(jnp.bfloat16)
    return grad_input, grad_up, grad_down
```

```python
import functools

import jax
import jax.numpy as jnp
from jax import lax
from jax.experimental import pallas as pl
from jax.experimental.pallas import tpu as pltpu
from jax.sharding import Mesh, PartitionSpec as P

LW = 1536
QW = 768
BF = jnp.bfloat16
F32 = jnp.float32
ALL = ("dp", "zl", "y", "x", "core")
GROUP = ("zl", "y", "x", "core")
PLANE = ("y", "x", "core")
ANY = pl.BlockSpec(memory_space=pl.ANY)
SMEM = pl.BlockSpec(memory_space=pltpu.SMEM)
VLIMIT = 62 * 1024 * 1024


def iota(shape, dim):
    return lax.broadcasted_iota(jnp.int32, shape, dim)


def onehot(cond):
    return jnp.where(cond, 1.0, 0.0).astype(BF)


def dot_nn(left, right):
    return lax.dot_general(left, right, (((1,), (0,)), ((), ())), preferred_element_type=F32)


def dot_nt(left, right):
    return lax.dot_general(left, right, (((1,), (1,)), ((), ())), preferred_element_type=F32)


def dot_tn(left, right):
    return lax.dot_general(left, right, (((0,), (0,)), ((), ())), preferred_element_type=F32)


def rank_rows(ids, weights, first, experts):
    top, tokens = ids.shape
    index = iota((experts, tokens), 0) + first
    member = jnp.zeros((experts, tokens), F32)
    weight = jnp.zeros((experts, tokens), F32)
    for k in range(top):
        hit = ids[k : k + 1, :] == index
        member = member + jnp.where(hit, 1.0, 0.0)
        weight = weight + jnp.where(hit, weights[k : k + 1, :], 0.0)
    before = onehot(iota((tokens, tokens), 0) < iota((tokens, tokens), 1))
    rank = member * (dot_nn(member.astype(BF), before) + 1.0)
    spread = onehot(iota((experts * 8, experts), 0) // 8 == iota((experts * 8, experts), 1))
    w1 = weight.astype(BF)
    rest = weight - w1.astype(F32)
    w2 = rest.astype(BF)
    w3 = (rest - w2.astype(F32)).astype(BF)
    low = dot_nn(spread, w2) + dot_nn(spread, w3)
    return dot_nn(spread, rank.astype(BF)), dot_nn(spread, w1) + low


def padded(piece):
    if piece.shape[0] == LW:
        return piece
    return jnp.concatenate([piece, jnp.zeros((LW - piece.shape[0], piece.shape[1]), piece.dtype)], axis=0)


def row_weight(hit, weight):
    return jnp.sum(jnp.where(hit, weight, 0.0), axis=1, keepdims=True)


def pack_own_body(ids_ref, w_ref, x_ref, dy_ref, out_ref, rank_ref, weight_s):
    step = pl.program_id(0)
    rows, tokens = rank_ref.shape
    width = x_ref.shape[0]

    @pl.when(step == 0)
    def _():
        rank, weight = rank_rows(ids_ref[...], w_ref[...], 0, rows // 8)
        rank_ref[...] = rank
        weight_s[...] = weight

    slot = iota((rows, tokens), 0) % 8
    pieces = ((x_ref, 0, LW), (x_ref, LW, width - LW), (dy_ref, 0, LW), (dy_ref, LW, width - LW))
    for g in range(4):

        @pl.when(step == g)
        def _(g=g):
            ref, start, size = pieces[g]
            hit = rank_ref[...] == (slot + 1).astype(F32)
            value = dot_nt(onehot(hit), padded(ref[pl.ds(start, size), :]))
            if g >= 2:
                value = value * row_weight(hit, weight_s[...])
            out_ref[...] = value.reshape(rows // 8, 1, 8, LW).astype(BF)

    @pl.when(step == 4)
    def _():
        hit = rank_ref[...] == (slot % 2 + 9).astype(F32)
        which = slot // 2
        picks = jnp.concatenate([onehot(hit & (which == c)) for c in range(4)], axis=1)
        source = jnp.concatenate([padded(ref[pl.ds(start, size), :]) for ref, start, size in pieces], axis=1)
        value = dot_nt(picks, source)
        scale = jnp.where(which[:, :1] >= 2, row_weight(hit, weight_s[...]), 1.0)
        out_ref[...] = (value * scale).reshape(rows // 8, 1, 8, LW).astype(BF)


def pack_own(ids, weights, x, dy, peers):
    tokens = ids.shape[1]
    whole = lambda a: pl.BlockSpec(a.shape, lambda g: (0, 0))
    return pl.pallas_call(
        pack_own_body,
        grid=(5,),
        in_specs=[whole(ids), whole(weights), whole(x), whole(dy)],
        out_specs=[
            pl.BlockSpec((peers, 1, 8, LW), lambda g: (0, g, 0, 0)),
            pl.BlockSpec((peers * 8, tokens), lambda g: (0, 0)),
        ],
        out_shape=[
            jax.ShapeDtypeStruct((peers, 5, 8, LW), BF),
            jax.ShapeDtypeStruct((peers * 8, tokens), F32),
        ],
        scratch_shapes=[pltpu.VMEM((peers * 8, tokens), F32)],
        compiler_params=pltpu.CompilerParams(vmem_limit_bytes=VLIMIT),
        name="pack_own",
    )(ids, weights, x, dy)


def pack_other_body(zl_ref, pa_ref, pb_ref, ma_ref, mb_ref, out_ref, rank_s, weight_s):
    step = pl.program_id(0)
    _, rows, tokens = rank_s.shape
    top = ma_ref.shape[0] // 2
    half = pa_ref.shape[0] // 3

    @pl.when(step == 0)
    def _():
        for s, meta in enumerate((ma_ref, mb_ref)):
            ids = meta[pl.ds(0, top), :].astype(jnp.int32)
            rank, weight = rank_rows(ids, meta[pl.ds(top, top), :], zl_ref[0] * (rows // 8), rows // 8)
            rank_s[s] = rank
            weight_s[s] = weight

    slot = iota((rows, tokens), 0) % 8
    spans = ((half, LW), (half + LW, 2 * half - LW), (0, half))
    pays = (pa_ref, pb_ref)
    for c in range(3):
        for s in range(2):

            @pl.when(step == c * 2 + s)
            def _(c=c, s=s):
                start, size = spans[c]
                hit = rank_s[s] == (slot + 1).astype(F32)
                value = dot_nt(onehot(hit), padded(pays[s][pl.ds(start, size), :]))
                if c < 2:
                    value = value * row_weight(hit, weight_s[s])
                out_ref[...] = value.reshape(rows // 8, 1, 8, LW).astype(BF)

    def remainder(pieces, per_piece):
        picks, source = [], []
        scale = jnp.zeros((rows, 1), F32)
        for s in range(2):
            hit = rank_s[s] == (slot % 2 + 9).astype(F32)
            scale = scale + jnp.where((slot[:, :1] // 2) % 2 == s, row_weight(hit, weight_s[s]), 0.0)
            for n, c in enumerate(pieces):
                mine = hit & (slot // 2 == n * 2 + s)
                picks.append(onehot(mine))
                start, size = spans[c]
                source.append(padded(pays[s][pl.ds(start, size), :]))
        value = dot_nt(jnp.concatenate(picks, axis=1), jnp.concatenate(source, axis=1))
        if per_piece:
            value = value * scale
        out_ref[...] = value.reshape(rows // 8, 1, 8, LW).astype(BF)

    @pl.when(step == 6)
    def _():
        remainder((0, 1), True)

    @pl.when(step == 7)
    def _():
        remainder((2,), False)


def pack_other(zl, pay_a, pay_b, meta_a, meta_b, peers):
    tokens = meta_a.shape[1]
    whole = lambda a: pl.BlockSpec(a.shape, lambda g: (0, 0))
    return pl.pallas_call(
        pack_other_body,
        grid=(8,),
        in_specs=[SMEM, whole(pay_a), whole(pay_b), whole(meta_a), whole(meta_b)],
        out_specs=pl.BlockSpec((peers, 1, 8, LW), lambda g: (0, g, 0, 0)),
        out_shape=jax.ShapeDtypeStruct((peers, 8, 8, LW), BF),
        scratch_shapes=[pltpu.VMEM((2, peers * 8, tokens), F32), pltpu.VMEM((2, peers * 8, tokens), F32)],
        compiler_params=pltpu.CompilerParams(vmem_limit_bytes=VLIMIT),
        name="pack_other",
    )(zl, pay_a, pay_b, meta_a, meta_b)


def blocks(total, size):
    return [(start, min(size, total - start)) for start in range(0, total, size)]


def expert_body(
    dp_ref, slab, wup, wdn, ret_o, gp_o, keep_o, send_o, xh_o, dy_o,
    x3, dy3, xr, dyr, rem, wu, wd, act_s, gp_s, keep_s, send_s, xh_s, ret, rest, sems, osems,
):
    peers = slab.shape[0]
    main = peers * 8
    rows = main + peers * 2
    hidden, width = wu.shape
    copies = [
        pltpu.make_async_copy(src, dst, sems.at[i])
        for i, (src, dst) in enumerate(
            (
                (slab.at[:, 0], x3.at[pl.ds(0, peers), :, pl.ds(0, LW)]),
                (slab.at[:, 1], xr),
                (slab.at[:, 4], rem),
                (wup, wu),
                (slab.at[:, 2], dy3.at[pl.ds(0, peers), :, pl.ds(0, LW)]),
                (slab.at[:, 3], dyr),
                (wdn, wd),
            )
        )
    ]
    for copy in copies:
        copy.start()
    right = width - LW
    for i in range(3):
        copies[i].wait()
    x3[pl.ds(0, peers), :, pl.ds(LW, right)] = xr[:, :, pl.ds(0, right)]
    last = rem[...].reshape(main, LW)
    r_i = iota((peers * 2, main), 0)
    c_i = iota((peers * 2, main), 1)
    for c in range(4):
        pick = onehot(c_i == (r_i // 2) * 8 + 2 * c + r_i % 2)
        dst = (x3, dy3)[c // 2]
        start, size = ((0, LW), (LW, right))[c % 2]
        value = dot_nn(pick, last[:, :size])
        dst[pl.ds(peers, peers // 4), :, pl.ds(start, size)] = value.reshape(peers // 4, 8, size).astype(BF)
    for i in range(3, 7):
        copies[i].wait()
    dy3[pl.ds(0, peers), :, pl.ds(LW, right)] = dyr[:, :, pl.ds(0, right)]
    out_dy = pltpu.make_async_copy(dy3, dy_o, osems.at[0])
    out_dy.start()
    for start, size in blocks(hidden, 512):
        pre = dot_nt(x3[...].reshape(rows, width), wu[pl.ds(start, size), :])
        s = jax.nn.sigmoid(pre)
        act_s[:, pl.ds(start, size)] = (pre * s).astype(BF)
        slope = s * (1.0 + pre * (1.0 - s))
        grad = dot_nt(dy3[...].reshape(rows, width), wd[pl.ds(start, size), :])
        gp_s[:, pl.ds(start, size)] = (grad * slope).astype(BF)
    out_gp = pltpu.make_async_copy(gp_s, gp_o, osems.at[1])
    out_gp.start()
    first = dp_ref[0] == 0
    a0 = act_s[:, pl.ds(0, hidden // 2)]
    a1 = act_s[:, pl.ds(hidden // 2, hidden // 2)]
    keep_s[...] = jnp.where(first, a0, a1)
    send_s[...] = jnp.where(first, a1, a0)
    out_keep = pltpu.make_async_copy(keep_s, keep_o, osems.at[2])
    out_send = pltpu.make_async_copy(send_s, send_o, osems.at[3])
    out_keep.start()
    out_send.start()
    x0 = x3[:, :, pl.ds(0, width // 2)]
    x1 = x3[:, :, pl.ds(width // 2, width // 2)]
    xh_s[...] = jnp.where(first, x0, x1)
    out_xh = pltpu.make_async_copy(xh_s, xh_o, osems.at[4])
    out_xh.start()
    outs = [out_dy, out_gp, out_keep, out_send, out_xh]
    rest[...] = jnp.zeros(rest.shape, F32)
    r_j = iota((main, peers * 2), 0)
    c_j = iota((main, peers * 2), 1)
    for q, (start, size) in enumerate(blocks(width, QW)):
        value = dot_nn(gp_s[...], wu[:, pl.ds(start, size)]).astype(BF)
        head = value[:main].reshape(peers, 8, size)
        if size < QW:
            ret[:, q] = jnp.zeros((peers, 8, QW), BF)
        ret[:, q, :, pl.ds(0, size)] = head
        place = onehot(((r_j % 8) // 2 == q) & (c_j == (r_j // 8) * 2 + r_j % 2))
        rest[:, pl.ds(0, size)] = rest[:, pl.ds(0, size)] + dot_nn(place, value[main:])
        copy = pltpu.make_async_copy(ret.at[:, q], ret_o.at[:, q], osems.at[5 + q])
        copy.start()
        outs.append(copy)
    ret[:, 4] = rest[...].reshape(peers, 8, QW).astype(BF)
    copy = pltpu.make_async_copy(ret.at[:, 4], ret_o.at[:, 4], osems.at[9])
    copy.start()
    outs.append(copy)
    for copy in outs:
        copy.wait()


def expert(dp, slab, wup, wdn):
    peers = slab.shape[0]
    hidden, width = wup.shape
    rows = peers * 10
    tiles = rows // 8
    sds = jax.ShapeDtypeStruct
    return pl.pallas_call(
        expert_body,
        in_specs=[SMEM, ANY, ANY, ANY],
        out_specs=[ANY] * 6,
        out_shape=[
            sds((peers, 5, 8, QW), BF),
            sds((rows, hidden), BF),
            sds((rows, hidden // 2), BF),
            sds((rows, hidden // 2), BF),
            sds((tiles, 8, width // 2), BF),
            sds((tiles, 8, width), BF),
        ],
        scratch_shapes=[
            pltpu.VMEM((tiles, 8, width), BF),
            pltpu.VMEM((tiles, 8, width), BF),
            pltpu.VMEM((peers, 8, LW), BF),
            pltpu.VMEM((peers, 8, LW), BF),
            pltpu.VMEM((peers, 8, LW), BF),
            pltpu.VMEM((hidden, width), BF),
            pltpu.VMEM((hidden, width), BF),
            pltpu.VMEM((rows, hidden), BF),
            pltpu.VMEM((rows, hidden), BF),
            pltpu.VMEM((rows, hidden // 2), BF),
            pltpu.VMEM((rows, hidden // 2), BF),
            pltpu.VMEM((tiles, 8, width // 2), BF),
            pltpu.VMEM((peers, 5, 8, QW), BF),
            pltpu.VMEM((peers * 8, QW), F32),
            pltpu.SemaphoreType.DMA((7,)),
            pltpu.SemaphoreType.DMA((10,)),
        ],
        compiler_params=pltpu.CompilerParams(vmem_limit_bytes=VLIMIT),
        cost_estimate=pl.CostEstimate(flops=6 * rows * hidden * width, transcendentals=rows * hidden, bytes_accessed=40_000_000),
        name="expert",
    )(dp, slab, wup, wdn)


def unpack_body(zl_ref, slab, dy_o, xh_o, dy3, xh3, dyr, xhr, r6, r7, sems):
    plane = slab.shape[0]
    peers = plane * 2
    width = dy3.shape[2]
    half = width // 2
    right = width - LW
    zl = zl_ref[0]
    copies = []
    for z in range(2):
        rel = lax.bitwise_xor(zl, z)
        span = pl.ds(z * plane, plane)
        copies.append(pltpu.make_async_copy(slab.at[:, rel], dy3.at[span, :, pl.ds(0, LW)], sems.at[3 * z]))
        copies.append(pltpu.make_async_copy(slab.at[:, 2 + rel], dyr.at[span], sems.at[3 * z + 1]))
        copies.append(pltpu.make_async_copy(slab.at[:, 4 + rel], xhr.at[span], sems.at[3 * z + 2]))
    copies.append(pltpu.make_async_copy(slab.at[:, 6], r6, sems.at[6]))
    copies.append(pltpu.make_async_copy(slab.at[:, 7], r7, sems.at[7]))
    for copy in copies:
        copy.start()
    for copy in copies:
        copy.wait()
    dy3[pl.ds(0, peers), :, pl.ds(LW, right)] = dyr[:, :, pl.ds(0, right)]
    xh3[pl.ds(0, peers)] = xhr[:, :, pl.ds(0, half)]
    r_i = iota((peers * 2, plane * 8), 0)
    c_i = iota((peers * 2, plane * 8), 1)
    rel = lax.bitwise_xor(r_i // peers, zl)
    base = ((r_i // 2) % plane) * 8 + rel * 2 + r_i % 2
    for c in range(3):
        source = (r6 if c < 2 else r7)[...].reshape(plane * 8, LW)
        size = (LW, right, half)[c]
        value = dot_nn(onehot(c_i == base + (4 if c == 1 else 0)), source[:, :size])
        value = value.reshape(peers // 4, 8, size).astype(BF)
        if c < 2:
            dy3[pl.ds(peers, peers // 4), :, pl.ds(c * LW, size)] = value
        else:
            xh3[pl.ds(peers, peers // 4)] = value
    outs = [
        pltpu.make_async_copy(dy3, dy_o, sems.at[8]),
        pltpu.make_async_copy(xh3, xh_o, sems.at[9]),
    ]
    for copy in outs:
        copy.start()
    for copy in outs:
        copy.wait()


def unpack_other(zl, slab, width):
    plane = slab.shape[0]
    peers = plane * 2
    tiles = peers * 10 // 8
    sds = jax.ShapeDtypeStruct
    return pl.pallas_call(
        unpack_body,
        in_specs=[SMEM, ANY],
        out_specs=[ANY, ANY],
        out_shape=[sds((tiles, 8, width), BF), sds((tiles, 8, width // 2), BF)],
        scratch_shapes=[
            pltpu.VMEM((tiles, 8, width), BF),
            pltpu.VMEM((tiles, 8, width // 2), BF),
            pltpu.VMEM((peers, 8, LW), BF),
            pltpu.VMEM((peers, 8, LW), BF),
            pltpu.VMEM((plane, 8, LW), BF),
            pltpu.VMEM((plane, 8, LW), BF),
            pltpu.SemaphoreType.DMA((10,)),
        ],
        compiler_params=pltpu.CompilerParams(vmem_limit_bytes=VLIMIT),
        name="unpack_other",
    )(zl, slab)


def combine_body(rank_ref, ret_ref, out_ref):
    peers = ret_ref.shape[0]
    rows, tokens = rank_ref.shape
    width = out_ref.shape[0]
    slot = iota((rows, tokens), 0) % 8
    rank = rank_ref[...]
    main = onehot(rank == (slot + 1).astype(F32))
    last = rank == (slot % 2 + 9).astype(F32)
    for q, (start, size) in enumerate(blocks(width, QW)):
        pick = jnp.concatenate([main, onehot(last & (slot // 2 == q))], axis=0)
        got = jnp.concatenate([ret_ref[:, q].reshape(rows, QW), ret_ref[:, 4].reshape(rows, QW)], axis=0)
        value = dot_tn(pick, got[:, :size])
        out_ref[pl.ds(start, size), :] = value.T.astype(BF)


def combine(rank, ret, width):
    return pl.pallas_call(
        combine_body,
        out_shape=jax.ShapeDtypeStruct((width, rank.shape[1]), BF),
        compiler_params=pltpu.CompilerParams(vmem_limit_bytes=VLIMIT),
        name="combine",
    )(rank, ret)


def local(sizes, tokens_in, grad_out, expert_ids, combine_weights, up_weight, down_weight):
    n_dp, n_zl, n_plane = sizes
    peers = n_zl * n_plane
    width = tokens_in.shape[1]
    half = width // 2
    x = tokens_in.T
    dy = grad_out.T
    ids = expert_ids.T
    weights = combine_weights.T
    dp = lax.axis_index("dp").astype(jnp.int32)
    zl = lax.axis_index("zl").astype(jnp.int32)

    def other(value, flip):
        pairs = []
        for i in range(n_dp * peers):
            d, z, p = i // peers, (i // n_plane) % n_zl, i % n_plane
            pairs.append((i, ((1 - d) * n_zl + (z ^ flip)) * n_plane + p))
        return lax.ppermute(value, ALL, pairs)

    pay = jnp.concatenate([lax.dynamic_slice_in_dim(x, (1 - dp) * half, half, 0), dy], axis=0)
    meta = jnp.concatenate([ids.astype(F32), weights], axis=0)
    meta_a, meta_b = other(meta, 0), other(meta, 1)
    pay_a, pay_b = other(pay, 0), other(pay, 1)

    slab, rank = pack_own(ids, weights, x, dy, peers)
    got = lax.all_to_all(slab, GROUP, 0, 0, tiled=True)
    slab_other = pack_other(zl[None], pay_a, pay_b, meta_a, meta_b, n_plane)
    got_other = lax.all_to_all(slab_other, PLANE, 0, 0, tiled=True)

    ret, gp, act, act_send, xh, dyr = expert(dp[None], got, up_weight[0].T, down_weight[0])
    back = lax.all_to_all(ret, GROUP, 0, 0, tiled=True)
    gp_other = other(gp, 0)
    act_other = other(act_send, 0)
    dy_other, xh_other = unpack_other(zl[None], got_other, width)

    flat = lambda a: a.reshape(-1, a.shape[-1])
    grad_up = dot_tn(flat(xh), gp) + dot_tn(flat(xh_other), gp_other)
    grad_down = dot_tn(act, flat(dyr)) + dot_tn(act_other, flat(dy_other))
    grad_input = combine(rank, back, width).T
    return (grad_input, grad_up.astype(BF)[None], grad_down.astype(BF)[None])


def build(devices, shape):
    n_dp, n_zl, n_y, n_x, n_core = shape
    fine = Mesh(devices.reshape(shape), ALL)
    token = P(ALL, None)
    weight = P(GROUP, None, None)
    return jax.shard_map(
        functools.partial(local, (n_dp, n_zl, n_y * n_x * n_core)),
        mesh=fine,
        in_specs=(token, token, token, token, weight, weight),
        out_specs=(token, P(GROUP, "dp", None), P(GROUP, "dp", None)),
        check_vma=False,
    )


def solution(mesh):
    return build(mesh.devices, (2, 2, 4, 4, 2))
```

```python
import functools

import jax
import jax.numpy as jnp
from jax import lax
from jax.experimental import pallas as pl
from jax.experimental.pallas import tpu as pltpu
from jax.sharding import Mesh, PartitionSpec as P


LW = 1536
QW = 768
BF = jnp.bfloat16
F32 = jnp.float32
ALL = ("dp", "zl", "y", "x", "core")
GROUP = ("zl", "y", "x", "core")
PLANE = ("y", "x", "core")
ANY = pl.BlockSpec(memory_space=pl.ANY)
SMEM = pl.BlockSpec(memory_space=pltpu.SMEM)
VLIMIT = 62 * 1024 * 1024


def iota(shape, dim):
    return lax.broadcasted_iota(jnp.int32, shape, dim)


def onehot(cond):
    return jnp.where(cond, 1.0, 0.0).astype(BF)


def dot_nn(left, right):
    return lax.dot_general(left, right, (((1,), (0,)), ((), ())), preferred_element_type=F32)


def dot_nt(left, right):
    return lax.dot_general(left, right, (((1,), (1,)), ((), ())), preferred_element_type=F32)


def dot_tn(left, right):
    return lax.dot_general(left, right, (((0,), (0,)), ((), ())), preferred_element_type=F32)


def rank_rows(ids, parts, first, experts):
    top, tokens = ids.shape
    index = iota((experts, tokens), 0) + first
    member = jnp.zeros((experts, tokens), F32)
    weight = [jnp.zeros((experts, tokens), F32) for _ in parts]
    for k in range(top):
        hit = ids[k : k + 1, :] == index
        member = member + jnp.where(hit, 1.0, 0.0)
        weight = [w + jnp.where(hit, part[k : k + 1, :], 0.0) for w, part in zip(weight, parts)]
    before = onehot(iota((tokens, tokens), 0) < iota((tokens, tokens), 1))
    rank = member * (dot_nn(member.astype(BF), before) + 1.0)
    spread = onehot(iota((experts * 8, experts), 0) // 8 == iota((experts * 8, experts), 1))
    total = None
    for w in reversed(weight):
        piece = dot_nn(spread, w.astype(BF))
        total = piece if total is None else piece + total
    return dot_nn(spread, rank.astype(BF)), total


def padded(piece, width):
    if piece.shape[0] == width:
        return piece
    return jnp.concatenate([piece, jnp.zeros((width - piece.shape[0], piece.shape[1]), piece.dtype)], axis=0)


def row_weight(hit, weight):
    return jnp.sum(jnp.where(hit, weight, 0.0), axis=1, keepdims=True)


def blocks(total, size):
    return [(start, min(size, total - start)) for start in range(0, total, size)]


def pack_x_body(ids_ref, w_ref, x_ref, out_ref, rank_ref, meta_ref):
    step = pl.program_id(0)
    rows, tokens = rank_ref.shape

    @pl.when(step == 0)
    def _():
        rank, _ = rank_rows(ids_ref[...], [], 0, rows // 8)
        rank_ref[...] = rank
        meta_ref[...] = jnp.concatenate([ids_ref[...].astype(F32), w_ref[...]], axis=0)

    slot = iota((rows, tokens), 0) % 8
    pieces = blocks(x_ref.shape[0], QW)
    for q, (start, size) in enumerate(pieces):

        @pl.when(step == q)
        def _(start=start, size=size):
            hit = rank_ref[...] == (slot + 1).astype(F32)
            value = dot_nt(onehot(hit), padded(x_ref[pl.ds(start, size), :], QW))
            out_ref[...] = value.reshape(rows // 8, 1, 8, QW).astype(BF)

    @pl.when(step == 4)
    def _():
        hit = rank_ref[...] == (slot % 2 + 9).astype(F32)
        picks = jnp.concatenate([onehot(hit & (slot // 2 == q)) for q in range(4)], axis=1)
        source = jnp.concatenate([padded(x_ref[pl.ds(start, size), :], QW) for start, size in pieces], axis=1)
        out_ref[...] = dot_nt(picks, source).reshape(rows // 8, 1, 8, QW).astype(BF)


def pack_x(ids, weights, x, peers):
    tokens = ids.shape[1]
    whole = lambda a: pl.BlockSpec(a.shape, lambda g: (0, 0))
    return pl.pallas_call(
        pack_x_body,
        grid=(5,),
        in_specs=[whole(ids), whole(weights), whole(x)],
        out_specs=[
            pl.BlockSpec((peers, 1, 8, QW), lambda g: (0, g, 0, 0)),
            pl.BlockSpec((peers * 8, tokens), lambda g: (0, 0)),
            pl.BlockSpec((2 * ids.shape[0], tokens), lambda g: (0, 0)),
        ],
        out_shape=[
            jax.ShapeDtypeStruct((peers, 5, 8, QW), BF),
            jax.ShapeDtypeStruct((peers * 8, tokens), F32),
            jax.ShapeDtypeStruct((2 * ids.shape[0], tokens), F32),
        ],
        compiler_params=pltpu.CompilerParams(vmem_limit_bytes=VLIMIT),
        name="pack_x",
    )(ids, weights, x)


def pack_dy_body(spans, zl_ref, pa_ref, pb_ref, ma_ref, mb_ref, out_ref, rank_s, weight_s):
    step = pl.program_id(0)
    _, rows, tokens = rank_s.shape
    pays = (pa_ref, pb_ref)
    top = ma_ref.shape[0] // 2

    @pl.when(step == 0)
    def _():
        for s, meta in enumerate((ma_ref, mb_ref)):
            ids = meta[pl.ds(0, top), :].astype(jnp.int32)
            weight = meta[pl.ds(top, top), :]
            w1 = weight.astype(BF)
            rest = weight - w1.astype(F32)
            w2 = rest.astype(BF)
            w3 = (rest - w2.astype(F32)).astype(BF)
            parts = [w.astype(F32) for w in (w1, w2, w3)]
            rank, weight = rank_rows(ids, parts, zl_ref[0] * (rows // 8), rows // 8)
            rank_s[s] = rank
            weight_s[s] = weight

    slot = iota((rows, tokens), 0) % 8
    for c, (start, size) in enumerate(spans):
        for s in range(2):

            @pl.when(step == c * 2 + s)
            def _(start=start, size=size, s=s):
                hit = rank_s[s] == (slot + 1).astype(F32)
                value = dot_nt(onehot(hit), padded(pays[s][pl.ds(start, size), :], LW))
                value = value * row_weight(hit, weight_s[s])
                out_ref[...] = value.reshape(rows // 8, 1, 8, LW).astype(BF)

    @pl.when(step == 4)
    def _():
        picks, source = [], []
        scale = jnp.zeros((rows, 1), F32)
        for s in range(2):
            hit = rank_s[s] == (slot % 2 + 9).astype(F32)
            scale = scale + jnp.where((slot[:, :1] // 2) % 2 == s, row_weight(hit, weight_s[s]), 0.0)
            for c, (start, size) in enumerate(spans):
                picks.append(onehot(hit & (slot // 2 == c * 2 + s)))
                source.append(padded(pays[s][pl.ds(start, size), :], LW))
        value = dot_nt(jnp.concatenate(picks, axis=1), jnp.concatenate(source, axis=1))
        out_ref[...] = (value * scale).reshape(rows // 8, 1, 8, LW).astype(BF)


def pack_dy(zl, dy_a, dy_b, meta_a, meta_b, peers):
    width, tokens = dy_a.shape
    spans = ((0, LW), (LW, width - LW))
    whole = lambda a: pl.BlockSpec(a.shape, lambda g: (0, 0))
    return pl.pallas_call(
        functools.partial(pack_dy_body, spans),
        grid=(5,),
        in_specs=[SMEM, whole(dy_a), whole(dy_b), whole(meta_a), whole(meta_b)],
        out_specs=pl.BlockSpec((peers, 1, 8, LW), lambda g: (0, g, 0, 0)),
        out_shape=jax.ShapeDtypeStruct((peers, 5, 8, LW), BF),
        scratch_shapes=[pltpu.VMEM((2, peers * 8, tokens), F32), pltpu.VMEM((2, peers * 8, tokens), F32)],
        compiler_params=pltpu.CompilerParams(vmem_limit_bytes=VLIMIT),
    )(zl, dy_a, dy_b, meta_a, meta_b)


def load_plane(zl, slab, first, dst, tmp, sems):
    plane = slab.shape[0]
    copies = []
    for z in range(2):
        rel = lax.bitwise_xor(zl, z)
        span = pl.ds(z * plane, plane)
        copies.append(pltpu.make_async_copy(slab.at[:, first + rel], dst.at[span, :, pl.ds(0, LW)], sems.at[2 * z]))
        copies.append(pltpu.make_async_copy(slab.at[:, first + 2 + rel], tmp.at[span], sems.at[2 * z + 1]))
    for copy in copies:
        copy.start()
    return copies


def rem_rows(zl, last, piece, size):
    plane = last.shape[0]
    peers = plane * 2
    r_i = iota((peers * 2, plane * 8), 0)
    c_i = iota((peers * 2, plane * 8), 1)
    rel = lax.bitwise_xor(r_i // peers, zl)
    base = ((r_i // 2) % plane) * 8 + piece * 4 + rel * 2 + r_i % 2
    value = dot_nn(onehot(c_i == base), last[...].reshape(plane * 8, LW)[:, :size])
    return value.reshape(peers // 4, 8, size).astype(BF)


def pre_body(dp_ref, slab, wup, act_o, slope_o, xh_o, xs_o, x3, xq, rem, wu, act_s, slope_s, xh_s, xs_s, sems, osems):
    peers = slab.shape[0]
    main = peers * 8
    rows = main + peers * 2
    hidden, width = wu.shape
    pieces = blocks(width, QW)
    copies = [pltpu.make_async_copy(wup, wu, sems.at[5])]
    for q, (start, size) in enumerate(pieces):
        dst = xq if size < QW else x3.at[pl.ds(0, peers), :, pl.ds(start, QW)]
        copies.append(pltpu.make_async_copy(slab.at[:, q], dst, sems.at[q]))
    copies.append(pltpu.make_async_copy(slab.at[:, 4], rem, sems.at[4]))
    for copy in copies:
        copy.start()
    for copy in copies[1:]:
        copy.wait()
    start, size = pieces[-1]
    x3[pl.ds(0, peers), :, pl.ds(start, size)] = xq[:, :, pl.ds(0, size)]
    last = rem[...].reshape(main, QW)
    r_i = iota((peers * 2, main), 0)
    c_i = iota((peers * 2, main), 1)
    for q, (start, size) in enumerate(pieces):
        pick = onehot(c_i == (r_i // 2) * 8 + 2 * q + r_i % 2)
        value = dot_nn(pick, last[:, :size])
        x3[pl.ds(peers, peers // 4), :, pl.ds(start, size)] = value.reshape(peers // 4, 8, size).astype(BF)
    copies[0].wait()
    first = dp_ref[0] == 0
    x0 = x3[:, :, pl.ds(0, width // 2)]
    x1 = x3[:, :, pl.ds(width // 2, width // 2)]
    xh_s[...] = jnp.where(first, x0, x1)
    xs_s[...] = jnp.where(first, x1, x0)
    outs = [pltpu.make_async_copy(xh_s, xh_o, osems.at[0]), pltpu.make_async_copy(xs_s, xs_o, osems.at[1])]
    outs[0].start()
    outs[1].start()
    for start, size in blocks(hidden, 512):
        pre = dot_nt(x3[...].reshape(rows, width), wu[pl.ds(start, size), :])
        s = jax.nn.sigmoid(pre)
        act_s[pl.ds(start, size), :] = (pre * s).T.astype(BF)
        slope_s[:, pl.ds(start, size)] = s * (1.0 + pre * (1.0 - s))
    copy = pltpu.make_async_copy(slope_s, slope_o, osems.at[3])
    copy.start()
    outs.append(copy)
    copy = pltpu.make_async_copy(act_s, act_o, osems.at[2])
    copy.start()
    outs.append(copy)
    for copy in outs:
        copy.wait()


def expert_pre(dp, slab, wup):
    peers = slab.shape[0]
    hidden, width = wup.shape
    rows = peers * 10
    tiles = rows // 8
    sds = jax.ShapeDtypeStruct
    return pl.pallas_call(
        pre_body,
        in_specs=[SMEM, ANY, ANY],
        out_specs=[ANY] * 4,
        out_shape=[sds((hidden, rows), BF), sds((rows, hidden), F32)] + [sds((tiles, 8, width // 2), BF)] * 2,
        scratch_shapes=[
            pltpu.VMEM((tiles, 8, width), BF),
            pltpu.VMEM((peers, 8, QW), BF),
            pltpu.VMEM((peers, 8, QW), BF),
            pltpu.VMEM((hidden, width), BF),
            pltpu.VMEM((hidden, rows), BF),
            pltpu.VMEM((rows, hidden), F32),
            pltpu.VMEM((tiles, 8, width // 2), BF),
            pltpu.VMEM((tiles, 8, width // 2), BF),
            pltpu.SemaphoreType.DMA((6,)),
            pltpu.SemaphoreType.DMA((4,)),
        ],
        compiler_params=pltpu.CompilerParams(vmem_limit_bytes=VLIMIT),
        cost_estimate=pl.CostEstimate(flops=2 * rows * hidden * width, transcendentals=rows * hidden, bytes_accessed=20_000_000),
        name="expert_pre",
    )(dp, slab, wup)


def grad_body(zl_ref, slab, slope, wup, wdn, ret_o, gp_o, dy_o, dy3, dyr, rem, wu, wd, slope_s, gp_s, gpt_s, ret, rest, sems, osems):
    plane = slab.shape[0]
    peers = plane * 2
    main = peers * 8
    rows = main + peers * 2
    hidden, width = wu.shape
    right = width - LW
    zl = zl_ref[0]
    copies = load_plane(zl, slab, 0, dy3, dyr, sems)
    more = [
        pltpu.make_async_copy(src, dst, sems.at[4 + i])
        for i, (src, dst) in enumerate(((slab.at[:, 4], rem), (wdn, wd), (slope, slope_s), (wup, wu)))
    ]
    for copy in more:
        copy.start()
    for copy in copies + more[:1]:
        copy.wait()
    dy3[pl.ds(0, peers), :, pl.ds(LW, right)] = dyr[:, :, pl.ds(0, right)]
    for c, (start, size) in enumerate(((0, LW), (LW, right))):
        dy3[pl.ds(peers, peers // 4), :, pl.ds(start, size)] = rem_rows(zl, rem, c, size)
    outs = [pltpu.make_async_copy(dy3, dy_o, osems.at[0])]
    outs[0].start()
    for copy in more[1:3]:
        copy.wait()
    for start, size in blocks(hidden, 512):
        grad = dot_nt(dy3[...].reshape(rows, width), wd[pl.ds(start, size), :])
        value = (grad * slope_s[:, pl.ds(start, size)]).astype(BF)
        gp_s[:, pl.ds(start, size)] = value
        gpt_s[pl.ds(start, size), :] = value.T
    copy = pltpu.make_async_copy(gpt_s, gp_o, osems.at[1])
    copy.start()
    outs.append(copy)
    more[3].wait()
    rest[...] = jnp.zeros(rest.shape, F32)
    r_j = iota((main, peers * 2), 0)
    c_j = iota((main, peers * 2), 1)

    def columns(q, start, size):
        value = dot_nn(gp_s[...], wu[:, pl.ds(start, size)]).astype(BF)
        ret[:, q, :, pl.ds(0, size)] = value[:main].reshape(peers, 8, size)
        place = onehot(((r_j % 8) // 2 == q) & (c_j == (r_j // 8) * 2 + r_j % 2))
        rest[:, pl.ds(0, size)] = rest[:, pl.ds(0, size)] + dot_nn(place, value[main:])
        pltpu.make_async_copy(ret.at[:, q], ret_o.at[:, q], osems.at[2 + q]).start()

    full = width // QW
    ret[:, full] = jnp.zeros((peers, 8, QW), BF)
    lax.fori_loop(0, full, lambda q, c: (columns(q, pl.multiple_of(q * QW, QW), QW), c)[1], 0)
    columns(full, full * QW, width - full * QW)
    outs += [pltpu.make_async_copy(ret.at[:, q], ret_o.at[:, q], osems.at[2 + q]) for q in range(full + 1)]
    ret[:, 4] = rest[...].reshape(peers, 8, QW).astype(BF)
    copy = pltpu.make_async_copy(ret.at[:, 4], ret_o.at[:, 4], osems.at[6])
    copy.start()
    outs.append(copy)
    for copy in outs:
        copy.wait()


def expert_grad(zl, slab, slope, wup, wdn):
    plane = slab.shape[0]
    peers = plane * 2
    hidden, width = wup.shape
    rows = peers * 10
    tiles = rows // 8
    sds = jax.ShapeDtypeStruct
    return pl.pallas_call(
        grad_body,
        in_specs=[SMEM, ANY, ANY, ANY, ANY],
        out_specs=[ANY] * 3,
        out_shape=[sds((peers, 5, 8, QW), BF), sds((hidden, rows), BF), sds((tiles, 8, width), BF)],
        scratch_shapes=[
            pltpu.VMEM((tiles, 8, width), BF),
            pltpu.VMEM((peers, 8, LW), BF),
            pltpu.VMEM((plane, 8, LW), BF),
            pltpu.VMEM((hidden, width), BF),
            pltpu.VMEM((hidden, width), BF),
            pltpu.VMEM(slope.shape, F32),
            pltpu.VMEM((rows, hidden), BF),
            pltpu.VMEM((hidden, rows), BF),
            pltpu.VMEM((peers, 5, 8, QW), BF),
            pltpu.VMEM((peers * 8, QW), F32),
            pltpu.SemaphoreType.DMA((8,)),
            pltpu.SemaphoreType.DMA((7,)),
        ],
        compiler_params=pltpu.CompilerParams(vmem_limit_bytes=VLIMIT),
        cost_estimate=pl.CostEstimate(flops=4 * rows * hidden * width, transcendentals=0, bytes_accessed=40_000_000),
        name="expert_grad",
    )(zl, slab, slope, wup, wdn)


def unpack_body(zl_ref, slab, dy_o, dy3, dyr, rem, sems):
    plane = slab.shape[0]
    peers = plane * 2
    width = dy3.shape[2]
    right = width - LW
    zl = zl_ref[0]
    copies = load_plane(zl, slab, 0, dy3, dyr, sems)
    copies.append(pltpu.make_async_copy(slab.at[:, 4], rem, sems.at[4]))
    copies[-1].start()
    for copy in copies:
        copy.wait()
    dy3[pl.ds(0, peers), :, pl.ds(LW, right)] = dyr[:, :, pl.ds(0, right)]
    for c, (start, size) in enumerate(((0, LW), (LW, right))):
        dy3[pl.ds(peers, peers // 4), :, pl.ds(start, size)] = rem_rows(zl, rem, c, size)
    copy = pltpu.make_async_copy(dy3, dy_o, sems.at[5])
    copy.start()
    copy.wait()


def unpack_other(zl, slab, width):
    plane = slab.shape[0]
    peers = plane * 2
    tiles = peers * 10 // 8
    return pl.pallas_call(
        unpack_body,
        in_specs=[SMEM, ANY],
        out_specs=ANY,
        out_shape=jax.ShapeDtypeStruct((tiles, 8, width), BF),
        scratch_shapes=[
            pltpu.VMEM((tiles, 8, width), BF),
            pltpu.VMEM((peers, 8, LW), BF),
            pltpu.VMEM((plane, 8, LW), BF),
            pltpu.SemaphoreType.DMA((6,)),
        ],
        compiler_params=pltpu.CompilerParams(vmem_limit_bytes=VLIMIT),
        name="unpack_other",
    )(zl, slab)


def combine_body(rank_ref, ret_ref, last_ref, out_ref, rem_s):
    step = pl.program_id(0)
    rows, tokens = rank_ref.shape
    slot = iota((rows, tokens), 0) % 8
    rank = rank_ref[...]

    @pl.when(step == 0)
    def _():
        last = rank == (slot % 2 + 9).astype(F32)
        picks = jnp.concatenate([onehot(last & (slot // 2 == q)) for q in range(4)], axis=1)
        rem_s[...] = dot_tn(picks, last_ref[...].reshape(rows, QW)).reshape(4, tokens, QW)

    value = dot_tn(onehot(rank == (slot + 1).astype(F32)), ret_ref[...].reshape(rows, QW)) + rem_s[step]
    out_ref[...] = value.T.astype(BF)


def combine(rank, ret, width):
    peers = ret.shape[0]
    return pl.pallas_call(
        combine_body,
        grid=(4,),
        in_specs=[
            pl.BlockSpec(rank.shape, lambda q: (0, 0)),
            pl.BlockSpec((peers, 1, 8, QW), lambda q: (0, q, 0, 0)),
            pl.BlockSpec((peers, 1, 8, QW), lambda q: (0, 4, 0, 0)),
        ],
        out_specs=pl.BlockSpec((QW, rank.shape[1]), lambda q: (q, 0)),
        out_shape=jax.ShapeDtypeStruct((width, rank.shape[1]), BF),
        scratch_shapes=[pltpu.VMEM((4, rank.shape[1], QW), F32)],
        compiler_params=pltpu.CompilerParams(vmem_limit_bytes=VLIMIT),
        name="combine",
    )(rank, ret, ret)


def local(sizes, tokens_in, grad_out, expert_ids, combine_weights, up_weight, down_weight):
    n_dp, n_zl, n_plane = sizes
    peers = n_zl * n_plane
    width = tokens_in.shape[1]
    x = tokens_in.T
    dy = grad_out.T
    ids = expert_ids.T
    weights = combine_weights.T
    wup = up_weight[0].T
    wdn = down_weight[0]
    dp = lax.axis_index("dp").astype(jnp.int32)
    zl = lax.axis_index("zl").astype(jnp.int32)

    def move(value, cross, flip):
        pairs = []
        for i in range(n_dp * peers):
            d, z, p = i // peers, (i // n_plane) % n_zl, i % n_plane
            pairs.append((i, ((d ^ cross) * n_zl + (z ^ flip)) * n_plane + p))
        return lax.ppermute(value, ALL, pairs)

    slab, rank, meta = pack_x(ids, weights, x, peers)
    dy_near = move(dy, 0, 1)
    meta_near = move(meta, 0, 1)
    dy_a, meta_a = move(dy, 1, 0), move(meta, 1, 0)
    dy_b, meta_b = move(dy, 1, 1), move(meta, 1, 1)

    got_x = lax.all_to_all(slab, GROUP, 0, 0, tiled=True)
    slab_dy = pack_dy(zl[None], dy, dy_near, meta, meta_near, n_plane)
    got_dy = lax.all_to_all(slab_dy, PLANE, 0, 0, tiled=True)
    slab_other = pack_dy(zl[None], dy_a, dy_b, meta_a, meta_b, n_plane)
    got_other = lax.all_to_all(slab_other, PLANE, 0, 0, tiled=True)

    act, slope, xh, x_send = expert_pre(dp[None], got_x, wup)
    xh_other = move(x_send, 1, 0)
    act_keep = lax.dynamic_slice_in_dim(act, dp * (act.shape[0] // 2), act.shape[0] // 2, 0)
    act_send = lax.dynamic_slice_in_dim(act, (1 - dp) * (act.shape[0] // 2), act.shape[0] // 2, 0)
    act_other = move(act_send, 1, 0)
    ret, gp, dyr = expert_grad(zl[None], got_dy, slope, wup, wdn)
    gp_other = move(gp, 1, 0)
    back = lax.all_to_all(ret, GROUP, 0, 0, tiled=True)
    dy_other = unpack_other(zl[None], got_other, width)

    flat = lambda a: a.reshape(-1, a.shape[-1])
    up = lambda a, b: lax.dot_general(a, b, (((0,), (1,)), ((), ())), preferred_element_type=F32)
    grad_down = (dot_nn(act_keep, flat(dyr)) + dot_nn(act_other, flat(dy_other))).astype(BF)[None]
    grad_up = (up(flat(xh_other), gp_other) + up(flat(xh), gp)).astype(BF)[None]
    grad_input = combine(rank, back, width).T
    return grad_input, grad_up, grad_down


def build(devices, shape):
    n_dp, n_zl, n_y, n_x, n_core = shape
    fine = Mesh(devices.reshape(shape), ALL)
    token = P(ALL, None)
    weight = P(GROUP, None, None)
    inner = functools.partial(local, (n_dp, n_zl, n_y * n_x * n_core))

    return jax.shard_map(
        inner,
        mesh=fine,
        in_specs=(token, token, token, token, weight, weight),
        out_specs=(token, P(GROUP, "dp", None), P(GROUP, "dp", None)),
        check_vma=False,
    )


def solution(mesh):
    return build(mesh.devices, (2, 2, 4, 4, 2))
```

```python
import functools

import jax
import jax.numpy as jnp
from jax import lax
from jax.experimental import pallas as pl
from jax.experimental.pallas import tpu as pltpu
from jax.sharding import Mesh, PartitionSpec as P


LW = 1536
QW = 768
LANES = 128
BF = jnp.bfloat16
F32 = jnp.float32
ALL = ("dp", "zl", "y", "x", "core")
GROUP = ("zl", "y", "x", "core")
PLANE = ("y", "x", "core")
ANY = pl.BlockSpec(memory_space=pl.ANY)
SMEM = pl.BlockSpec(memory_space=pltpu.SMEM)
VLIMIT = 62 * 1024 * 1024


def iota(shape, dim):
    return lax.broadcasted_iota(jnp.int32, shape, dim)


def onehot(cond):
    return jnp.where(cond, 1.0, 0.0).astype(BF)


def dot_nn(left, right):
    return lax.dot_general(left, right, (((1,), (0,)), ((), ())), preferred_element_type=F32)


def dot_nt(left, right):
    return lax.dot_general(left, right, (((1,), (1,)), ((), ())), preferred_element_type=F32)


def dot_tn(left, right):
    return lax.dot_general(left, right, (((0,), (0,)), ((), ())), preferred_element_type=F32)


def rank_rows(ids, parts, first, experts):
    top, tokens = ids.shape
    index = iota((experts, tokens), 0) + first
    member = jnp.zeros((experts, tokens), F32)
    weight = [jnp.zeros((experts, tokens), F32) for _ in parts]
    for k in range(top):
        hit = ids[k : k + 1, :] == index
        member = member + jnp.where(hit, 1.0, 0.0)
        weight = [w + jnp.where(hit, part[k : k + 1, :], 0.0) for w, part in zip(weight, parts)]
    before = onehot(iota((tokens, tokens), 0) < iota((tokens, tokens), 1))
    rank = member * (dot_nn(member.astype(BF), before) + 1.0)
    spread = onehot(iota((experts * 8, experts), 0) // 8 == iota((experts * 8, experts), 1))
    total = None
    for w in reversed(weight):
        piece = dot_nn(spread, w.astype(BF))
        total = piece if total is None else piece + total
    return dot_nn(spread, rank.astype(BF)), total


def padded(piece, width):
    if piece.shape[0] == width:
        return piece
    return jnp.concatenate([piece, jnp.zeros((width - piece.shape[0], piece.shape[1]), piece.dtype)], axis=0)


def row_weight(hit, weight):
    return jnp.sum(jnp.where(hit, weight, 0.0), axis=1, keepdims=True)


def blocks(total, size):
    return [(start, min(size, total - start)) for start in range(0, total, size)]


def tiles(width):
    return -(-width // LANES)


def from_tiles(ref, first, count):
    peers = ref.shape[0]
    return jnp.concatenate([ref[:, first + i].reshape(peers * 8, LANES) for i in range(count)], axis=1)


def to_tiles(ref, first, value):
    rows, width = value.shape
    for i in range(tiles(width)):
        part = value[:, i * LANES : min(width, (i + 1) * LANES)]
        ref[:, first + i, :, pl.ds(0, part.shape[1])] = part.reshape(rows // 8, 8, part.shape[1]).astype(BF)


def pack_x_body(ids_ref, w_ref, x_ref, out_o, rank_ref, meta_ref, out_s, sems):
    rows, tokens = rank_ref.shape
    rank, _ = rank_rows(ids_ref[...], [], 0, rows // 8)
    rank_ref[...] = rank
    meta_ref[...] = jnp.concatenate([ids_ref[...].astype(F32), w_ref[...]], axis=0)
    slot = iota((rows, tokens), 0) % 8
    width = x_ref.shape[0]
    pieces = blocks(width, QW)
    spans = [(start // LANES, tiles(size)) for start, size in pieces] + [(tiles(width), tiles(QW))]
    copies = [
        pltpu.make_async_copy(out_s.at[:, pl.ds(c, n)], out_o.at[:, pl.ds(c, n)], sems.at[g])
        for g, (c, n) in enumerate(spans)
    ]
    main = onehot(rank == (slot + 1).astype(F32))
    for q, (start, size) in enumerate(pieces):
        to_tiles(out_s, spans[q][0], dot_nt(main, padded(x_ref[pl.ds(start, size), :], spans[q][1] * LANES)))
        copies[q].start()
    hit = rank == (slot % 2 + 9).astype(F32)
    picks = jnp.concatenate([onehot(hit & (slot // 2 == q)) for q in range(4)], axis=1)
    source = jnp.concatenate([padded(x_ref[pl.ds(start, size), :], QW) for start, size in pieces], axis=1)
    to_tiles(out_s, spans[4][0], dot_nt(picks, source))
    copies[4].start()
    for copy in copies:
        copy.wait()


def pack_x(ids, weights, x, peers):
    tokens = ids.shape[1]
    count = tiles(x.shape[0]) + tiles(QW)
    vmem = pl.BlockSpec(memory_space=pltpu.VMEM)
    return pl.pallas_call(
        pack_x_body,
        in_specs=[vmem, vmem, vmem],
        out_specs=[ANY, vmem, vmem],
        out_shape=[
            jax.ShapeDtypeStruct((peers, count, 8, LANES), BF),
            jax.ShapeDtypeStruct((peers * 8, tokens), F32),
            jax.ShapeDtypeStruct((2 * ids.shape[0], tokens), F32),
        ],
        scratch_shapes=[pltpu.VMEM((peers, count, 8, LANES), BF), pltpu.SemaphoreType.DMA((5,))],
        compiler_params=pltpu.CompilerParams(vmem_limit_bytes=VLIMIT),
        name="pack_x",
    )(ids, weights, x)


def pack_dy_body(zl_ref, pa_ref, pb_ref, ma_ref, mb_ref, out_o, out_s, sems):
    width, tokens = pa_ref.shape
    peers = out_s.shape[0]
    rows = peers * 8
    top = ma_ref.shape[0] // 2
    pays = (pa_ref, pb_ref)
    slot = iota((rows, tokens), 0) % 8
    spans = blocks(width, LW)
    ranks, scales = [], []
    for meta in (ma_ref, mb_ref):
        ids = meta[pl.ds(0, top), :].astype(jnp.int32)
        weight = meta[pl.ds(top, top), :]
        w1 = weight.astype(BF)
        rest = weight - w1.astype(F32)
        w2 = rest.astype(BF)
        w3 = (rest - w2.astype(F32)).astype(BF)
        parts = [w.astype(F32) for w in (w1, w2, w3)]
        rank, weight = rank_rows(ids, parts, zl_ref[0] * peers, peers)
        ranks.append(rank)
        scales.append(weight)
    copies = []

    def send(first, value):
        to_tiles(out_s, first, value)
        part = pl.ds(first, tiles(value.shape[1]))
        copies.append(pltpu.make_async_copy(out_s.at[:, part], out_o.at[:, part], sems.at[len(copies)]))
        copies[-1].start()

    for s in range(2):
        hit = ranks[s] == (slot + 1).astype(F32)
        scale = row_weight(hit, scales[s])
        for start, size in spans:
            count = tiles(size)
            first = 2 * (start // LANES) + s * count
            send(first, dot_nt(onehot(hit), padded(pays[s][pl.ds(start, size), :], count * LANES)) * scale)
    picks, source = [], []
    scale = jnp.zeros((rows, 1), F32)
    for s in range(2):
        hit = ranks[s] == (slot % 2 + 9).astype(F32)
        scale = scale + jnp.where((slot[:, :1] // 2) % 2 == s, row_weight(hit, scales[s]), 0.0)
        for c, (start, size) in enumerate(spans):
            picks.append(onehot(hit & (slot // 2 == c * 2 + s)))
            source.append(padded(pays[s][pl.ds(start, size), :], LW))
    send(2 * tiles(width), dot_nt(jnp.concatenate(picks, axis=1), jnp.concatenate(source, axis=1)) * scale)
    for copy in copies:
        copy.wait()


def pack_dy(zl, dy_a, dy_b, meta_a, meta_b, peers):
    width = dy_a.shape[0]
    shape = (peers, 2 * tiles(width) + tiles(LW), 8, LANES)
    vmem = pl.BlockSpec(memory_space=pltpu.VMEM)
    return pl.pallas_call(
        pack_dy_body,
        in_specs=[SMEM, vmem, vmem, vmem, vmem],
        out_specs=ANY,
        out_shape=jax.ShapeDtypeStruct(shape, BF),
        scratch_shapes=[pltpu.VMEM(shape, BF), pltpu.SemaphoreType.DMA((5,))],
        compiler_params=pltpu.CompilerParams(vmem_limit_bytes=VLIMIT),
    )(zl, dy_a, dy_b, meta_a, meta_b)


def load_plane(zl, slab, main, rem, sems):
    plane = slab.shape[0]
    count = main.shape[1]
    left = tiles(LW)
    right = count - left
    copies = []
    for z in range(2):
        rel = lax.bitwise_xor(zl, z)
        span = pl.ds(z * plane, plane)
        for i, (first, n) in enumerate(((rel * left, left), (2 * left + rel * right, right))):
            copies.append(
                pltpu.make_async_copy(
                    slab.at[:, pl.ds(first, n)], main.at[span, pl.ds(i * left, n)], sems.at[2 * z + i]
                )
            )
    copies.append(pltpu.make_async_copy(slab.at[:, pl.ds(2 * count, left)], rem, sems.at[4]))
    for copy in copies:
        copy.start()
    return copies


def place_main(main, dst):
    peers = main.shape[0]
    width = dst.shape[2]
    for c, (start, size) in enumerate(blocks(width, LANES)):
        dst[pl.ds(0, peers), :, pl.ds(start, size)] = main[:, c, :, pl.ds(0, size)]


def place_rem(zl, rem, dst):
    plane = rem.shape[0]
    peers = plane * 2
    last = from_tiles(rem, 0, rem.shape[1])
    r_i = iota((peers * 2, plane * 8), 0)
    c_i = iota((peers * 2, plane * 8), 1)
    rel = lax.bitwise_xor(r_i // peers, zl)
    base = ((r_i // 2) % plane) * 8 + rel * 2 + r_i % 2
    for c, (start, size) in enumerate(blocks(dst.shape[2], LW)):
        value = dot_nn(onehot(c_i == base + 4 * c), last[:, :size])
        dst[pl.ds(peers, peers // 4), :, pl.ds(start, size)] = value.reshape(peers // 4, 8, size).astype(BF)


def split_body(dp_ref, slab, x_o, xh_o, xs_o, got, x3, xh_s, xs_s, sems, osems):
    peers = slab.shape[0]
    main = peers * 8
    width = x3.shape[2]
    copy = pltpu.make_async_copy(slab, got, sems.at[0])
    copy.start()
    copy.wait()
    place_main(got, x3)
    last = from_tiles(got, tiles(width), tiles(QW))
    r_i = iota((peers * 2, main), 0)
    c_i = iota((peers * 2, main), 1)
    for q, (start, size) in enumerate(blocks(width, QW)):
        pick = onehot(c_i == (r_i // 2) * 8 + 2 * q + r_i % 2)
        value = dot_nn(pick, last[:, :size])
        x3[pl.ds(peers, peers // 4), :, pl.ds(start, size)] = value.reshape(peers // 4, 8, size).astype(BF)
    first = dp_ref[0] == 0
    x0 = x3[:, :, pl.ds(0, width // 2)]
    x1 = x3[:, :, pl.ds(width // 2, width // 2)]
    xs_s[...] = jnp.where(first, x1, x0)
    outs = [pltpu.make_async_copy(xs_s, xs_o, osems.at[0])]
    outs[0].start()
    outs.append(pltpu.make_async_copy(x3, x_o, osems.at[1]))
    outs[1].start()
    xh_s[...] = jnp.where(first, x0, x1)
    outs.append(pltpu.make_async_copy(xh_s, xh_o, osems.at[2]))
    outs[2].start()
    for copy in outs:
        copy.wait()


def split_x(dp, slab, width):
    peers = slab.shape[0]
    groups = peers * 10 // 8
    sds = jax.ShapeDtypeStruct
    half = (groups, 8, width // 2)
    return pl.pallas_call(
        split_body,
        in_specs=[SMEM, ANY],
        out_specs=[ANY] * 3,
        out_shape=[sds((groups, 8, width), BF), sds(half, BF), sds(half, BF)],
        scratch_shapes=[
            pltpu.VMEM(slab.shape, BF),
            pltpu.VMEM((groups, 8, width), BF),
            pltpu.VMEM(half, BF),
            pltpu.VMEM(half, BF),
            pltpu.SemaphoreType.DMA((1,)),
            pltpu.SemaphoreType.DMA((3,)),
        ],
        compiler_params=pltpu.CompilerParams(vmem_limit_bytes=VLIMIT),
        name="split_x",
    )(dp, slab)


def pre_body(x, wup, act_o, slope_o, x3, wu, act_s, slope_s, sems, osems):
    groups, _, width = x.shape
    rows = groups * 8
    hidden = wup.shape[0]
    spans = blocks(hidden, 512)
    copies = [pltpu.make_async_copy(x, x3, sems.at[0])]
    for n, (start, size) in enumerate(spans):
        copies.append(pltpu.make_async_copy(wup.at[pl.ds(start, size)], wu.at[pl.ds(start, size)], sems.at[1 + n]))
    for copy in copies:
        copy.start()
    copies[0].wait()
    for n, (start, size) in enumerate(spans):
        copies[1 + n].wait()
        pre = dot_nt(x3[...].reshape(rows, width), wu[pl.ds(start, size), :])
        s = jax.nn.sigmoid(pre)
        act_s[pl.ds(start, size), :] = (pre * s).T.astype(BF)
        slope_s[:, pl.ds(start, size)] = s * (1.0 + pre * (1.0 - s))
    outs = [
        pltpu.make_async_copy(act_s, act_o, osems.at[0]),
        pltpu.make_async_copy(slope_s, slope_o, osems.at[1]),
    ]
    for copy in outs:
        copy.start()
    for copy in outs:
        copy.wait()


def expert_pre(x, wup):
    groups, _, width = x.shape
    rows = groups * 8
    hidden = wup.shape[0]
    sds = jax.ShapeDtypeStruct
    return pl.pallas_call(
        pre_body,
        in_specs=[ANY, ANY],
        out_specs=[ANY] * 2,
        out_shape=[sds((hidden, rows), BF), sds((rows, hidden), F32)],
        scratch_shapes=[
            pltpu.VMEM((groups, 8, width), BF),
            pltpu.VMEM((hidden, width), BF),
            pltpu.VMEM((hidden, rows), BF),
            pltpu.VMEM((rows, hidden), F32),
            pltpu.SemaphoreType.DMA((1 + len(blocks(hidden, 512)),)),
            pltpu.SemaphoreType.DMA((2,)),
        ],
        compiler_params=pltpu.CompilerParams(vmem_limit_bytes=VLIMIT),
        cost_estimate=pl.CostEstimate(flops=2 * rows * hidden * width, transcendentals=rows * hidden, bytes_accessed=20_000_000),
        name="expert_pre",
    )(x, wup)


def grad_body(zl_ref, slab, slope, wup, wdn, ret_o, gp_o, dy_o, got, rem, dy3, wu, wd, slope_s, gp_s, gpt_s, ret, rest, sems, osems):
    plane = slab.shape[0]
    peers = plane * 2
    main = peers * 8
    rows = main + peers * 2
    hidden, width = wu.shape
    zl = zl_ref[0]
    copies = load_plane(zl, slab, got, rem, sems)
    more = [
        pltpu.make_async_copy(src, dst, sems.at[5 + i])
        for i, (src, dst) in enumerate(((wdn, wd), (slope, slope_s), (wup, wu)))
    ]
    for copy in more:
        copy.start()
    for copy in copies:
        copy.wait()
    place_main(got, dy3)
    place_rem(zl, rem, dy3)
    outs = [pltpu.make_async_copy(dy3, dy_o, osems.at[0])]
    outs[0].start()
    for copy in more[:2]:
        copy.wait()
    for start, size in blocks(hidden, 512):
        grad = dot_nt(dy3[...].reshape(rows, width), wd[pl.ds(start, size), :])
        value = (grad * slope_s[:, pl.ds(start, size)]).astype(BF)
        gp_s[:, pl.ds(start, size)] = value
        gpt_s[pl.ds(start, size), :] = value.T
    copy = pltpu.make_async_copy(gpt_s, gp_o, osems.at[1])
    copy.start()
    outs.append(copy)
    more[2].wait()
    rest[...] = jnp.zeros(rest.shape, F32)
    r_j = iota((main, peers * 2), 0)
    c_j = iota((main, peers * 2), 1)

    def columns(q, start, size):
        value = dot_nn(gp_s[...], wu[:, pl.ds(start, size)]).astype(BF)
        to_tiles(ret, q * tiles(QW), value[:main])
        place = onehot(((r_j % 8) // 2 == q) & (c_j == (r_j // 8) * 2 + r_j % 2))
        rest[:, pl.ds(0, size)] = rest[:, pl.ds(0, size)] + dot_nn(place, value[main:])

    def send(q, first, count):
        part = pl.ds(first, count)
        return pltpu.make_async_copy(ret.at[:, part], ret_o.at[:, part], osems.at[2 + q])

    def step(q, carry):
        columns(q, pl.multiple_of(q * QW, QW), QW)
        send(q, q * tiles(QW), tiles(QW)).start()
        return carry

    full = width // QW
    end = width - full * QW
    ret[:, tiles(width) - 1] = jnp.zeros((peers, 8, LANES), BF)
    lax.fori_loop(0, full, step, 0)
    columns(full, full * QW, end)
    send(full, full * tiles(QW), tiles(end)).start()
    to_tiles(ret, tiles(width), rest[...])
    send(full + 1, tiles(width), tiles(QW)).start()
    outs += [send(q, q * tiles(QW), tiles(QW)) for q in range(full)]
    outs += [send(full, full * tiles(QW), tiles(end)), send(full + 1, tiles(width), tiles(QW))]
    for copy in outs:
        copy.wait()


def expert_grad(zl, slab, slope, wup, wdn):
    plane = slab.shape[0]
    peers = plane * 2
    hidden, width = wup.shape
    rows = peers * 10
    groups = rows // 8
    count = tiles(width) + tiles(QW)
    sds = jax.ShapeDtypeStruct
    return pl.pallas_call(
        grad_body,
        in_specs=[SMEM, ANY, ANY, ANY, ANY],
        out_specs=[ANY] * 3,
        out_shape=[sds((peers, count, 8, LANES), BF), sds((hidden, rows), BF), sds((groups, 8, width), BF)],
        scratch_shapes=[
            pltpu.VMEM((peers, tiles(width), 8, LANES), BF),
            pltpu.VMEM((plane, tiles(LW), 8, LANES), BF),
            pltpu.VMEM((groups, 8, width), BF),
            pltpu.VMEM((hidden, width), BF),
            pltpu.VMEM((hidden, width), BF),
            pltpu.VMEM(slope.shape, F32),
            pltpu.VMEM((rows, hidden), BF),
            pltpu.VMEM((hidden, rows), BF),
            pltpu.VMEM((peers, count, 8, LANES), BF),
            pltpu.VMEM((peers * 8, QW), F32),
            pltpu.SemaphoreType.DMA((8,)),
            pltpu.SemaphoreType.DMA((7,)),
        ],
        compiler_params=pltpu.CompilerParams(vmem_limit_bytes=VLIMIT),
        cost_estimate=pl.CostEstimate(flops=4 * rows * hidden * width, transcendentals=0, bytes_accessed=40_000_000),
        name="expert_grad",
    )(zl, slab, slope, wup, wdn)


def unpack_body(zl_ref, slab, dy_o, got, rem, dy3, sems):
    for copy in load_plane(zl_ref[0], slab, got, rem, sems):
        copy.wait()
    place_main(got, dy3)
    place_rem(zl_ref[0], rem, dy3)
    copy = pltpu.make_async_copy(dy3, dy_o, sems.at[5])
    copy.start()
    copy.wait()


def unpack_other(zl, slab, width):
    plane = slab.shape[0]
    peers = plane * 2
    groups = peers * 10 // 8
    return pl.pallas_call(
        unpack_body,
        in_specs=[SMEM, ANY],
        out_specs=ANY,
        out_shape=jax.ShapeDtypeStruct((groups, 8, width), BF),
        scratch_shapes=[
            pltpu.VMEM((peers, tiles(width), 8, LANES), BF),
            pltpu.VMEM((plane, tiles(LW), 8, LANES), BF),
            pltpu.VMEM((groups, 8, width), BF),
            pltpu.SemaphoreType.DMA((6,)),
        ],
        compiler_params=pltpu.CompilerParams(vmem_limit_bytes=VLIMIT),
        name="unpack_other",
    )(zl, slab)


def combine_body(rank_ref, ret_ref, out_ref, got, sems):
    rows, tokens = rank_ref.shape
    width = out_ref.shape[0]
    spans = [(tiles(width), tiles(QW))] + [(start // LANES, tiles(size)) for start, size in blocks(width, QW)]
    copies = [
        pltpu.make_async_copy(ret_ref.at[:, pl.ds(c, n)], got.at[:, pl.ds(c, n)], sems.at[i])
        for i, (c, n) in enumerate(spans)
    ]
    for copy in copies:
        copy.start()
    slot = iota((rows, tokens), 0) % 8
    rank = rank_ref[...]
    last = rank == (slot % 2 + 9).astype(F32)
    picks = jnp.concatenate([onehot(last & (slot // 2 == q)) for q in range(4)], axis=1)
    main = onehot(rank == (slot + 1).astype(F32))
    copies[0].wait()
    rem = dot_tn(picks, from_tiles(got, *spans[0]))
    for q, (start, size) in enumerate(blocks(width, QW)):
        copies[1 + q].wait()
        value = dot_tn(main, from_tiles(got, *spans[1 + q]))[:, :size]
        value = value + rem[q * tokens : (q + 1) * tokens, :size]
        out_ref[pl.ds(start, size), :] = value.T.astype(BF)


def combine(rank, ret, width):
    vmem = pl.BlockSpec(memory_space=pltpu.VMEM)
    return pl.pallas_call(
        combine_body,
        in_specs=[vmem, ANY],
        out_specs=vmem,
        out_shape=jax.ShapeDtypeStruct((width, rank.shape[1]), BF),
        scratch_shapes=[pltpu.VMEM(ret.shape, BF), pltpu.SemaphoreType.DMA((5,))],
        compiler_params=pltpu.CompilerParams(vmem_limit_bytes=VLIMIT),
        name="combine",
    )(rank, ret)


def local(sizes, tokens_in, grad_out, expert_ids, combine_weights, up_weight, down_weight):
    n_dp, n_zl, n_plane = sizes
    peers = n_zl * n_plane
    width = tokens_in.shape[1]
    x = tokens_in.T
    dy = grad_out.T
    ids = expert_ids.T
    weights = combine_weights.T
    wup = up_weight[0].T
    wdn = down_weight[0]
    dp = lax.axis_index("dp").astype(jnp.int32)
    zl = lax.axis_index("zl").astype(jnp.int32)

    def move(value, cross, flip):
        pairs = []
        for i in range(n_dp * peers):
            d, z, p = i // peers, (i // n_plane) % n_zl, i % n_plane
            pairs.append((i, ((d ^ cross) * n_zl + (z ^ flip)) * n_plane + p))
        return lax.ppermute(value, ALL, pairs)

    slab, rank, meta = pack_x(ids, weights, x, peers)
    dy_near = move(dy, 0, 1)
    meta_near = move(meta, 0, 1)
    dy_a, meta_a = move(dy, 1, 0), move(meta, 1, 0)
    dy_b, meta_b = move(dy, 1, 1), move(meta, 1, 1)

    got_x = lax.all_to_all(slab, GROUP, 0, 0, tiled=True)
    slab_dy = pack_dy(zl[None], dy, dy_near, meta, meta_near, n_plane)
    got_dy = lax.all_to_all(slab_dy, PLANE, 0, 0, tiled=True)
    slab_other = pack_dy(zl[None], dy_a, dy_b, meta_a, meta_b, n_plane)
    got_other = lax.all_to_all(slab_other, PLANE, 0, 0, tiled=True)

    x_rows, xh, x_send = split_x(dp[None], got_x, width)
    act, slope = expert_pre(x_rows, wup)
    xh_other = move(x_send, 1, 0)
    act_keep = lax.dynamic_slice_in_dim(act, dp * (act.shape[0] // 2), act.shape[0] // 2, 0)
    act_send = lax.dynamic_slice_in_dim(act, (1 - dp) * (act.shape[0] // 2), act.shape[0] // 2, 0)
    act_other = move(act_send, 1, 0)
    ret, gp, dyr = expert_grad(zl[None], got_dy, slope, wup, wdn)
    gp_other = move(gp, 1, 0)
    back = lax.all_to_all(ret, GROUP, 0, 0, tiled=True)
    dy_other = unpack_other(zl[None], got_other, width)

    flat = lambda a: a.reshape(-1, a.shape[-1])
    up = lambda a, b: lax.dot_general(a, b, (((0,), (1,)), ((), ())), preferred_element_type=F32)
    grad_down = (dot_nn(act_keep, flat(dyr)) + dot_nn(act_other, flat(dy_other))).astype(BF)[None]
    grad_up = (up(flat(xh_other), gp_other) + up(flat(xh), gp)).astype(BF)[None]
    grad_input = combine(rank, back, width).T
    return grad_input, grad_up, grad_down


def build(devices, shape):
    n_dp, n_zl, n_y, n_x, n_core = shape
    fine = Mesh(devices.reshape(shape), ALL)
    token = P(ALL, None)
    weight = P(GROUP, None, None)
    inner = functools.partial(local, (n_dp, n_zl, n_y * n_x * n_core))

    return jax.shard_map(
        inner,
        mesh=fine,
        in_specs=(token, token, token, token, weight, weight),
        out_specs=(token, P(GROUP, "dp", None), P(GROUP, "dp", None)),
        check_vma=False,
    )


def solution(mesh):
    return build(mesh.devices, (2, 2, 4, 4, 2))
```

```python
import functools

import jax
import jax.numpy as jnp
from jax import lax
from jax.experimental import pallas as pl
from jax.experimental.pallas import tpu as pltpu
from jax.sharding import Mesh, PartitionSpec as P


LW = 1536
QW = 768
LANES = 128
HB = 480
BF = jnp.bfloat16
F32 = jnp.float32
ALL = ("dp", "zl", "y", "x", "core")
GROUP = ("zl", "y", "x", "core")
PLANE = ("y", "x", "core")
ANY = pl.BlockSpec(memory_space=pl.ANY)
SMEM = pl.BlockSpec(memory_space=pltpu.SMEM)
VLIMIT = 62 * 1024 * 1024


def iota(shape, dim):
    return lax.broadcasted_iota(jnp.int32, shape, dim)


def onehot(cond):
    return jnp.where(cond, 1.0, 0.0).astype(BF)


def dot_nn(left, right):
    return lax.dot_general(left, right, (((1,), (0,)), ((), ())), preferred_element_type=F32)


def dot_nt(left, right):
    return lax.dot_general(left, right, (((1,), (1,)), ((), ())), preferred_element_type=F32)


def dot_tn(left, right):
    return lax.dot_general(left, right, (((0,), (0,)), ((), ())), preferred_element_type=F32)


def rank_rows(ids, parts, first, experts):
    top, tokens = ids.shape
    index = iota((experts, tokens), 0) + first
    member = jnp.zeros((experts, tokens), F32)
    weight = [jnp.zeros((experts, tokens), F32) for _ in parts]
    for k in range(top):
        hit = ids[k : k + 1, :] == index
        member = member + jnp.where(hit, 1.0, 0.0)
        weight = [w + jnp.where(hit, part[k : k + 1, :], 0.0) for w, part in zip(weight, parts)]
    before = onehot(iota((tokens, tokens), 0) < iota((tokens, tokens), 1))
    rank = member * (dot_nn(member.astype(BF), before) + 1.0)
    spread = onehot(iota((experts * 8, experts), 0) // 8 == iota((experts * 8, experts), 1))
    total = None
    for w in reversed(weight):
        piece = dot_nn(spread, w.astype(BF))
        total = piece if total is None else piece + total
    return dot_nn(spread, rank.astype(BF)), total


def padded(piece, width):
    if piece.shape[0] == width:
        return piece
    return jnp.concatenate([piece, jnp.zeros((width - piece.shape[0], piece.shape[1]), piece.dtype)], axis=0)


def row_weight(hit, weight):
    return jnp.sum(jnp.where(hit, weight, 0.0), axis=1, keepdims=True)


def blocks(total, size):
    return [(start, min(size, total - start)) for start in range(0, total, size)]


def parts(rows):
    return rows * 3 // 5


def tiles(width):
    return -(-width // LANES)


def from_tiles(ref, first, count):
    peers = ref.shape[0]
    return jnp.concatenate([ref[:, first + i].reshape(peers * 8, LANES) for i in range(count)], axis=1)


def to_tiles(ref, first, value):
    rows, width = value.shape
    for i in range(tiles(width)):
        part = value[:, i * LANES : min(width, (i + 1) * LANES)]
        ref[:, first + i, :, pl.ds(0, part.shape[1])] = part.reshape(rows // 8, 8, part.shape[1]).astype(BF)


def pack_x_body(ids_ref, w_ref, x_ref, out_o, rank_ref, meta_ref, out_s, sems):
    rows, tokens = rank_ref.shape
    rank, _ = rank_rows(ids_ref[...], [], 0, rows // 8)
    rank_ref[...] = rank
    meta_ref[...] = jnp.concatenate([ids_ref[...].astype(F32), w_ref[...]], axis=0)
    slot = iota((rows, tokens), 0) % 8
    width = x_ref.shape[0]
    pieces = blocks(width, QW)
    spans = [(start // LANES, tiles(size)) for start, size in pieces] + [(tiles(width), tiles(QW))]
    copies = [
        pltpu.make_async_copy(out_s.at[:, pl.ds(c, n)], out_o.at[:, pl.ds(c, n)], sems.at[g])
        for g, (c, n) in enumerate(spans)
    ]
    main = onehot(rank == (slot + 1).astype(F32))
    for q, (start, size) in enumerate(pieces):
        to_tiles(out_s, spans[q][0], dot_nt(main, padded(x_ref[pl.ds(start, size), :], spans[q][1] * LANES)))
        copies[q].start()
    hit = rank == (slot % 2 + 9).astype(F32)
    picks = jnp.concatenate([onehot(hit & (slot // 2 == q)) for q in range(4)], axis=1)
    source = jnp.concatenate([padded(x_ref[pl.ds(start, size), :], QW) for start, size in pieces], axis=1)
    to_tiles(out_s, spans[4][0], dot_nt(picks, source))
    copies[4].start()
    for copy in copies:
        copy.wait()


def pack_x(ids, weights, x, peers):
    tokens = ids.shape[1]
    count = tiles(x.shape[0]) + tiles(QW)
    vmem = pl.BlockSpec(memory_space=pltpu.VMEM)
    return pl.pallas_call(
        pack_x_body,
        in_specs=[vmem, vmem, vmem],
        out_specs=[ANY, vmem, vmem],
        out_shape=[
            jax.ShapeDtypeStruct((peers, count, 8, LANES), BF),
            jax.ShapeDtypeStruct((peers * 8, tokens), F32),
            jax.ShapeDtypeStruct((2 * ids.shape[0], tokens), F32),
        ],
        scratch_shapes=[pltpu.VMEM((peers, count, 8, LANES), BF), pltpu.SemaphoreType.DMA((5,))],
        compiler_params=pltpu.CompilerParams(vmem_limit_bytes=VLIMIT),
        name="pack_x",
    )(ids, weights, x)


def pack_dy_body(zl_ref, pa_ref, pb_ref, ma_ref, mb_ref, out_o, pay, meta, ranks, scales, out_s, sems, isems):
    _, width, tokens = pay.shape
    peers = out_s.shape[0]
    rows = peers * 8
    top = meta.shape[1] // 2
    loads = [
        pltpu.make_async_copy(src, dst.at[i % 2], isems.at[i])
        for i, (src, dst) in enumerate(((ma_ref, meta), (mb_ref, meta), (pa_ref, pay), (pb_ref, pay)))
    ]
    for copy in loads:
        copy.start()
    for copy in loads:
        copy.wait()
    slot = iota((rows, tokens), 0) % 8
    spans = blocks(width, LW)

    def send(i, first, count):
        part = pl.ds(first, count)
        return pltpu.make_async_copy(out_s.at[:, part], out_o.at[:, part], sems.at[i])

    def source(s, carry):
        ids = meta[s, pl.ds(0, top), :].astype(jnp.int32)
        weight = meta[s, pl.ds(top, top), :]
        w1 = weight.astype(BF)
        rest = weight - w1.astype(F32)
        w2 = rest.astype(BF)
        w3 = (rest - w2.astype(F32)).astype(BF)
        rank, weight = rank_rows(ids, [w.astype(F32) for w in (w1, w2, w3)], zl_ref[0] * peers, peers)
        ranks[s] = rank
        scales[s] = weight
        hit = rank == (slot + 1).astype(F32)
        scale = row_weight(hit, weight)
        for i, (start, size) in enumerate(spans):
            count = tiles(size)
            first = 2 * (start // LANES) + s * count
            to_tiles(out_s, first, dot_nt(onehot(hit), padded(pay[s, pl.ds(start, size), :], count * LANES)) * scale)
            send(2 * s + i, first, count).start()
        return carry

    lax.fori_loop(0, 2, source, 0)
    picks, pieces = [], []
    scale = jnp.zeros((rows, 1), F32)
    for s in range(2):
        hit = ranks[s] == (slot % 2 + 9).astype(F32)
        scale = scale + jnp.where((slot[:, :1] // 2) % 2 == s, row_weight(hit, scales[s]), 0.0)
        for c, (start, size) in enumerate(spans):
            picks.append(onehot(hit & (slot // 2 == c * 2 + s)))
            pieces.append(padded(pay[s, pl.ds(start, size), :], LW))
    last = 2 * tiles(width)
    to_tiles(out_s, last, dot_nt(jnp.concatenate(picks, axis=1), jnp.concatenate(pieces, axis=1)) * scale)
    send(4, last, tiles(LW)).start()
    for s in range(2):
        for i, (start, size) in enumerate(spans):
            send(2 * s + i, 2 * (start // LANES) + s * tiles(size), tiles(size)).wait()
    send(4, last, tiles(LW)).wait()


def pack_dy(zl, dy_a, dy_b, meta_a, meta_b, peers):
    width, tokens = dy_a.shape
    shape = (peers, 2 * tiles(width) + tiles(LW), 8, LANES)
    return pl.pallas_call(
        pack_dy_body,
        in_specs=[SMEM, ANY, ANY, ANY, ANY],
        out_specs=ANY,
        out_shape=jax.ShapeDtypeStruct(shape, BF),
        scratch_shapes=[
            pltpu.VMEM((2,) + dy_a.shape, BF),
            pltpu.VMEM((2,) + meta_a.shape, F32),
            pltpu.VMEM((2, peers * 8, tokens), F32),
            pltpu.VMEM((2, peers * 8, tokens), F32),
            pltpu.VMEM(shape, BF),
            pltpu.SemaphoreType.DMA((5,)),
            pltpu.SemaphoreType.DMA((4,)),
        ],
        compiler_params=pltpu.CompilerParams(vmem_limit_bytes=VLIMIT),
    )(zl, dy_a, dy_b, meta_a, meta_b)


def load_plane(zl, slab, main, rem, sems):
    plane = slab.shape[0]
    count = main.shape[1]
    left = tiles(LW)
    right = count - left
    copies = []
    for z in range(2):
        rel = lax.bitwise_xor(zl, z)
        span = pl.ds(z * plane, plane)
        for i, (first, n) in enumerate(((rel * left, left), (2 * left + rel * right, right))):
            copies.append(
                pltpu.make_async_copy(
                    slab.at[:, pl.ds(first, n)], main.at[span, pl.ds(i * left, n)], sems.at[2 * z + i]
                )
            )
    copies.append(pltpu.make_async_copy(slab.at[:, pl.ds(2 * count, left)], rem, sems.at[4]))
    for copy in copies:
        copy.start()
    return copies


def place_main(main, dst):
    peers = main.shape[0]
    width = dst.shape[2]
    for c, (start, size) in enumerate(blocks(width, LANES)):
        dst[pl.ds(0, peers), :, pl.ds(start, size)] = main[:, c, :, pl.ds(0, size)]


def place_rem(zl, rem, dst):
    plane = rem.shape[0]
    peers = plane * 2
    last = from_tiles(rem, 0, rem.shape[1])
    r_i = iota((peers * 2, plane * 8), 0)
    c_i = iota((peers * 2, plane * 8), 1)
    rel = lax.bitwise_xor(r_i // peers, zl)
    base = ((r_i // 2) % plane) * 8 + rel * 2 + r_i % 2
    for c, (start, size) in enumerate(blocks(dst.shape[2], LW)):
        value = dot_nn(onehot(c_i == base + 4 * c), last[:, :size])
        dst[pl.ds(peers, peers // 4), :, pl.ds(start, size)] = value.reshape(peers // 4, 8, size).astype(BF)


def split_body(dp_ref, slab, x_o, xh_o, xs_o, got, x3, xh_s, xs_s, sems, osems):
    peers = slab.shape[0]
    main = peers * 8
    width = x3.shape[2]
    copy = pltpu.make_async_copy(slab, got, sems.at[0])
    copy.start()
    copy.wait()
    place_main(got, x3)
    last = from_tiles(got, tiles(width), tiles(QW))
    r_i = iota((peers * 2, main), 0)
    c_i = iota((peers * 2, main), 1)
    for q, (start, size) in enumerate(blocks(width, QW)):
        pick = onehot(c_i == (r_i // 2) * 8 + 2 * q + r_i % 2)
        value = dot_nn(pick, last[:, :size])
        x3[pl.ds(peers, peers // 4), :, pl.ds(start, size)] = value.reshape(peers // 4, 8, size).astype(BF)
    first = dp_ref[0] == 0
    x0 = x3[:, :, pl.ds(0, width // 2)]
    x1 = x3[:, :, pl.ds(width // 2, width // 2)]
    xs_s[...] = jnp.where(first, x1, x0)
    outs = [pltpu.make_async_copy(xs_s, xs_o, osems.at[0])]
    outs[0].start()
    outs.append(pltpu.make_async_copy(x3, x_o, osems.at[1]))
    outs[1].start()
    xh_s[...] = jnp.where(first, x0, x1)
    outs.append(pltpu.make_async_copy(xh_s, xh_o, osems.at[2]))
    outs[2].start()
    for copy in outs:
        copy.wait()


def split_x(dp, slab, width):
    peers = slab.shape[0]
    groups = peers * 10 // 8
    sds = jax.ShapeDtypeStruct
    half = (groups, 8, width // 2)
    return pl.pallas_call(
        split_body,
        in_specs=[SMEM, ANY],
        out_specs=[ANY] * 3,
        out_shape=[sds((groups, 8, width), BF), sds(half, BF), sds(half, BF)],
        scratch_shapes=[
            pltpu.VMEM(slab.shape, BF),
            pltpu.VMEM((groups, 8, width), BF),
            pltpu.VMEM(half, BF),
            pltpu.VMEM(half, BF),
            pltpu.SemaphoreType.DMA((1,)),
            pltpu.SemaphoreType.DMA((3,)),
        ],
        compiler_params=pltpu.CompilerParams(vmem_limit_bytes=VLIMIT),
        name="split_x",
    )(dp, slab)


def pre_body(x, wup, act_o, slope_o, x3, wu, act_s, slope_s, sems, osems):
    groups, _, width = x.shape
    rows = groups * 8
    hidden = wup.shape[0]
    copies = [pltpu.make_async_copy(x, x3, sems.at[0]), pltpu.make_async_copy(wup, wu, sems.at[1])]
    for copy in copies:
        copy.start()
    for copy in copies:
        copy.wait()

    def block(n, carry):
        span = pl.ds(pl.multiple_of(n * HB, HB), HB)
        pre = dot_nt(x3[...].reshape(rows, width), wu[span, :])
        s = jax.nn.sigmoid(pre)
        act_s[span, :] = (pre * s).T.astype(BF)
        slope_s[n] = s * (1.0 + pre * (1.0 - s))
        return carry

    lax.fori_loop(0, hidden // HB, block, 0)
    outs = [
        pltpu.make_async_copy(act_s, act_o, osems.at[0]),
        pltpu.make_async_copy(slope_s, slope_o, osems.at[1]),
    ]
    for copy in outs:
        copy.start()
    for copy in outs:
        copy.wait()


def expert_pre(x, wup):
    groups, _, width = x.shape
    rows = groups * 8
    hidden = wup.shape[0]
    sds = jax.ShapeDtypeStruct
    return pl.pallas_call(
        pre_body,
        in_specs=[ANY, ANY],
        out_specs=[ANY] * 2,
        out_shape=[sds((hidden, rows), BF), sds((hidden // HB, rows, HB), F32)],
        scratch_shapes=[
            pltpu.VMEM((groups, 8, width), BF),
            pltpu.VMEM((hidden, width), BF),
            pltpu.VMEM((hidden, rows), BF),
            pltpu.VMEM((hidden // HB, rows, HB), F32),
            pltpu.SemaphoreType.DMA((2,)),
            pltpu.SemaphoreType.DMA((2,)),
        ],
        compiler_params=pltpu.CompilerParams(vmem_limit_bytes=VLIMIT),
        cost_estimate=pl.CostEstimate(flops=2 * rows * hidden * width, transcendentals=rows * hidden, bytes_accessed=20_000_000),
        name="expert_pre",
    )(x, wup)


def grad_body(zl_ref, slab, slope, wup, wdn, ret_o, gp_o, gpa_o, gpb_o, dy_o, got, rem, dy3, wu, wd, slope_s, gp_n, gp_s, gpt_s, ret, rest, sems, osems):
    plane = slab.shape[0]
    peers = plane * 2
    main = peers * 8
    rows = main + peers * 2
    hidden, width = wu.shape
    zl = zl_ref[0]
    copies = load_plane(zl, slab, got, rem, sems)
    more = [
        pltpu.make_async_copy(src, dst, sems.at[5 + i])
        for i, (src, dst) in enumerate(((wdn, wd), (slope, slope_s), (wup, wu)))
    ]
    for copy in more:
        copy.start()
    for copy in copies:
        copy.wait()
    place_main(got, dy3)
    place_rem(zl, rem, dy3)
    outs = [pltpu.make_async_copy(dy3, dy_o, osems.at[0])]
    outs[0].start()
    for copy in more[:2]:
        copy.wait()

    def block(n, carry):
        span = pl.ds(pl.multiple_of(n * HB, HB), HB)
        grad = dot_nt(dy3[...].reshape(rows, width), wd[span, :])
        value = (grad * slope_s[n]).astype(BF)
        gp_n[n] = value
        gpt_s[span, :] = value.T
        return carry

    lax.fori_loop(0, hidden // HB, block, 0)
    for n in range(hidden // HB):
        gp_s[:, pl.ds(n * HB, HB)] = gp_n[n]
    cut = gpa_o.shape[1]
    for i, (src, dst) in enumerate(
        (
            (gpt_s.at[:, pl.ds(0, cut)], gpa_o),
            (gpt_s.at[:, pl.ds(cut, rows - cut)], gpb_o),
            (gpt_s, gp_o),
        )
    ):
        outs.append(pltpu.make_async_copy(src, dst, osems.at[7 + i]))
        outs[-1].start()
    more[2].wait()
    rest[...] = jnp.zeros(rest.shape, F32)
    r_j = iota((main, peers * 2), 0)
    c_j = iota((main, peers * 2), 1)

    def columns(q, start, size):
        value = dot_nn(gp_s[...], wu[:, pl.ds(start, size)]).astype(BF)
        to_tiles(ret, q * tiles(QW), value[:main])
        place = onehot(((r_j % 8) // 2 == q) & (c_j == (r_j // 8) * 2 + r_j % 2))
        rest[:, pl.ds(0, size)] = rest[:, pl.ds(0, size)] + dot_nn(place, value[main:])

    def send(q, first, count):
        part = pl.ds(first, count)
        return pltpu.make_async_copy(ret.at[:, part], ret_o.at[:, part], osems.at[2 + q])

    def step(q, carry):
        columns(q, pl.multiple_of(q * QW, QW), QW)
        send(q, q * tiles(QW), tiles(QW)).start()
        return carry

    full = width // QW
    end = width - full * QW
    ret[:, tiles(width) - 1] = jnp.zeros((peers, 8, LANES), BF)
    lax.fori_loop(0, full, step, 0)
    columns(full, full * QW, end)
    send(full, full * tiles(QW), tiles(end)).start()
    to_tiles(ret, tiles(width), rest[...])
    send(full + 1, tiles(width), tiles(QW)).start()
    outs += [send(q, q * tiles(QW), tiles(QW)) for q in range(full)]
    outs += [send(full, full * tiles(QW), tiles(end)), send(full + 1, tiles(width), tiles(QW))]
    for copy in outs:
        copy.wait()


def expert_grad(zl, slab, slope, wup, wdn):
    plane = slab.shape[0]
    peers = plane * 2
    hidden, width = wup.shape
    rows = peers * 10
    groups = rows // 8
    cut = parts(rows)
    count = tiles(width) + tiles(QW)
    sds = jax.ShapeDtypeStruct
    return pl.pallas_call(
        grad_body,
        in_specs=[SMEM, ANY, ANY, ANY, ANY],
        out_specs=[ANY] * 5,
        out_shape=[sds((peers, count, 8, LANES), BF), sds((hidden, rows), BF)] + [sds((hidden, n), BF) for n in (cut, rows - cut)] + [sds((groups, 8, width), BF)],
        scratch_shapes=[
            pltpu.VMEM((peers, tiles(width), 8, LANES), BF),
            pltpu.VMEM((plane, tiles(LW), 8, LANES), BF),
            pltpu.VMEM((groups, 8, width), BF),
            pltpu.VMEM((hidden, width), BF),
            pltpu.VMEM((hidden, width), BF),
            pltpu.VMEM(slope.shape, F32),
            pltpu.VMEM(slope.shape, BF),
            pltpu.VMEM((rows, hidden), BF),
            pltpu.VMEM((hidden, rows), BF),
            pltpu.VMEM((peers, count, 8, LANES), BF),
            pltpu.VMEM((peers * 8, QW), F32),
            pltpu.SemaphoreType.DMA((8,)),
            pltpu.SemaphoreType.DMA((10,)),
        ],
        compiler_params=pltpu.CompilerParams(vmem_limit_bytes=VLIMIT),
        cost_estimate=pl.CostEstimate(flops=4 * rows * hidden * width, transcendentals=0, bytes_accessed=40_000_000),
        name="expert_grad",
    )(zl, slab, slope, wup, wdn)


def unpack_body(zl_ref, slab, dy_o, got, rem, dy3, sems):
    for copy in load_plane(zl_ref[0], slab, got, rem, sems):
        copy.wait()
    place_main(got, dy3)
    place_rem(zl_ref[0], rem, dy3)
    copy = pltpu.make_async_copy(dy3, dy_o, sems.at[5])
    copy.start()
    copy.wait()


def unpack_other(zl, slab, width):
    plane = slab.shape[0]
    peers = plane * 2
    groups = peers * 10 // 8
    return pl.pallas_call(
        unpack_body,
        in_specs=[SMEM, ANY],
        out_specs=ANY,
        out_shape=jax.ShapeDtypeStruct((groups, 8, width), BF),
        scratch_shapes=[
            pltpu.VMEM((peers, tiles(width), 8, LANES), BF),
            pltpu.VMEM((plane, tiles(LW), 8, LANES), BF),
            pltpu.VMEM((groups, 8, width), BF),
            pltpu.SemaphoreType.DMA((6,)),
        ],
        compiler_params=pltpu.CompilerParams(vmem_limit_bytes=VLIMIT),
        name="unpack_other",
    )(zl, slab)


def combine_body(rank_ref, ret_ref, out_o, got, out_ref, sems, osems):
    rows, tokens = rank_ref.shape
    width = out_ref.shape[0]
    outs = []
    spans = [(tiles(width), tiles(QW))] + [(start // LANES, tiles(size)) for start, size in blocks(width, QW)]
    copies = [
        pltpu.make_async_copy(ret_ref.at[:, pl.ds(c, n)], got.at[:, pl.ds(c, n)], sems.at[i])
        for i, (c, n) in enumerate(spans)
    ]
    for copy in copies:
        copy.start()
    slot = iota((rows, tokens), 0) % 8
    rank = rank_ref[...]
    last = rank == (slot % 2 + 9).astype(F32)
    picks = jnp.concatenate([onehot(last & (slot // 2 == q)) for q in range(4)], axis=1)
    main = onehot(rank == (slot + 1).astype(F32))
    copies[0].wait()
    rem = dot_tn(picks, from_tiles(got, *spans[0]))
    for q, (start, size) in enumerate(blocks(width, QW)):
        copies[1 + q].wait()
        value = dot_tn(main, from_tiles(got, *spans[1 + q]))[:, :size]
        value = value + rem[q * tokens : (q + 1) * tokens, :size]
        out_ref[pl.ds(start, size), :] = value.T.astype(BF)
        outs.append(pltpu.make_async_copy(out_ref.at[pl.ds(start, size)], out_o.at[pl.ds(start, size)], osems.at[q]))
        outs[-1].start()
    for copy in outs:
        copy.wait()


def combine(rank, ret, width):
    vmem = pl.BlockSpec(memory_space=pltpu.VMEM)
    return pl.pallas_call(
        combine_body,
        in_specs=[vmem, ANY],
        out_specs=ANY,
        out_shape=jax.ShapeDtypeStruct((width, rank.shape[1]), BF),
        scratch_shapes=[
            pltpu.VMEM(ret.shape, BF),
            pltpu.VMEM((width, rank.shape[1]), BF),
            pltpu.SemaphoreType.DMA((5,)),
            pltpu.SemaphoreType.DMA((4,)),
        ],
        compiler_params=pltpu.CompilerParams(vmem_limit_bytes=VLIMIT),
        name="combine",
    )(rank, ret)


def local(sizes, tokens_in, grad_out, expert_ids, combine_weights, up_weight, down_weight):
    n_dp, n_zl, n_plane = sizes
    peers = n_zl * n_plane
    width = tokens_in.shape[1]
    x = tokens_in.T
    dy = grad_out.T
    ids = expert_ids.T
    weights = combine_weights.T
    wup = up_weight[0].T
    wdn = down_weight[0]
    dp = lax.axis_index("dp").astype(jnp.int32)
    zl = lax.axis_index("zl").astype(jnp.int32)

    def move(value, cross, flip):
        pairs = []
        for i in range(n_dp * peers):
            d, z, p = i // peers, (i // n_plane) % n_zl, i % n_plane
            pairs.append((i, ((d ^ cross) * n_zl + (z ^ flip)) * n_plane + p))
        return lax.ppermute(value, ALL, pairs)

    slab, rank, meta = pack_x(ids, weights, x, peers)
    dy_near = move(dy, 0, 1)
    meta_near = move(meta, 0, 1)
    dy_a, meta_a = move(dy, 1, 0), move(meta, 1, 0)
    dy_b, meta_b = move(dy, 1, 1), move(meta, 1, 1)

    got_x = lax.all_to_all(slab, GROUP, 0, 0, tiled=True)
    slab_dy = pack_dy(zl[None], dy, dy_near, meta, meta_near, n_plane)
    got_dy = lax.all_to_all(slab_dy, PLANE, 0, 0, tiled=True)
    slab_other = pack_dy(zl[None], dy_a, dy_b, meta_a, meta_b, n_plane)
    got_other = lax.all_to_all(slab_other, PLANE, 0, 0, tiled=True)

    x_rows, xh, x_send = split_x(dp[None], got_x, width)
    act, slope = expert_pre(x_rows, wup)
    xh_other = move(x_send, 1, 0)
    act_keep = lax.dynamic_slice_in_dim(act, dp * (act.shape[0] // 2), act.shape[0] // 2, 0)
    act_send = lax.dynamic_slice_in_dim(act, (1 - dp) * (act.shape[0] // 2), act.shape[0] // 2, 0)
    act_other = move(act_send, 1, 0)
    ret, gp, gpa, gpb, dyr = expert_grad(zl[None], got_dy, slope, wup, wdn)
    gpa_other = move(gpa, 1, 0)
    gpb_other = move(gpb, 1, 0)
    back = lax.all_to_all(ret, GROUP, 0, 0, tiled=True)
    dy_other = unpack_other(zl[None], got_other, width)

    flat = lambda a: a.reshape(-1, a.shape[-1])
    up = lambda a, b: lax.dot_general(a, b, (((0,), (1,)), ((), ())), preferred_element_type=F32)
    grad_down = (dot_nn(act_keep, flat(dyr)) + dot_nn(act_other, flat(dy_other))).astype(BF)[None]
    cut = gpa.shape[1]
    xo = flat(xh_other)
    early = up(xo[:cut], gpa_other) + up(flat(xh), gp)
    grad_up = (up(xo[cut:], gpb_other) + early).astype(BF)[None]
    grad_input = combine(rank, back, width).T
    return grad_input, grad_up, grad_down


def build(devices, shape):
    n_dp, n_zl, n_y, n_x, n_core = shape
    fine = Mesh(devices.reshape(shape), ALL)
    token = P(ALL, None)
    weight = P(GROUP, None, None)
    inner = functools.partial(local, (n_dp, n_zl, n_y * n_x * n_core))

    return jax.shard_map(
        inner,
        mesh=fine,
        in_specs=(token, token, token, token, weight, weight),
        out_specs=(token, P(GROUP, "dp", None), P(GROUP, "dp", None)),
        check_vma=False,
    )


def solution(mesh):
    return build(mesh.devices, (2, 2, 4, 4, 2))
```

```python
import functools

import jax
import jax.numpy as jnp
from jax import lax
from jax.experimental import pallas as pl
from jax.experimental.pallas import tpu as pltpu
from jax.sharding import Mesh, PartitionSpec as P


LW = 1536
QW = 768
LANES = 128
HB = 480
BF = jnp.bfloat16
F32 = jnp.float32
ALL = ("dp", "zl", "y", "x", "core")
GROUP = ("zl", "y", "x", "core")
PLANE = ("y", "x", "core")
ANY = pl.BlockSpec(memory_space=pl.ANY)
SMEM = pl.BlockSpec(memory_space=pltpu.SMEM)
VLIMIT = 62 * 1024 * 1024


def iota(shape, dim):
    return lax.broadcasted_iota(jnp.int32, shape, dim)


def onehot(cond):
    return jnp.where(cond, 1.0, 0.0).astype(BF)


def dot_nn(left, right):
    return lax.dot_general(left, right, (((1,), (0,)), ((), ())), preferred_element_type=F32)


def dot_nt(left, right):
    return lax.dot_general(left, right, (((1,), (1,)), ((), ())), preferred_element_type=F32)


def dot_tn(left, right):
    return lax.dot_general(left, right, (((0,), (0,)), ((), ())), preferred_element_type=F32)


def rank_rows(ids, parts, first, experts):
    top, tokens = ids.shape
    index = iota((experts, tokens), 0) + first
    member = jnp.zeros((experts, tokens), F32)
    weight = [jnp.zeros((experts, tokens), F32) for _ in parts]
    for k in range(top):
        hit = ids[k : k + 1, :] == index
        member = member + jnp.where(hit, 1.0, 0.0)
        weight = [w + jnp.where(hit, part[k : k + 1, :], 0.0) for w, part in zip(weight, parts)]
    before = onehot(iota((tokens, tokens), 0) < iota((tokens, tokens), 1))
    rank = member * (dot_nn(member.astype(BF), before) + 1.0)
    spread = onehot(iota((experts * 8, experts), 0) // 8 == iota((experts * 8, experts), 1))
    total = None
    for w in reversed(weight):
        piece = dot_nn(spread, w.astype(BF))
        total = piece if total is None else piece + total
    return dot_nn(spread, rank.astype(BF)), total


def padded(piece, width):
    if piece.shape[0] == width:
        return piece
    return jnp.concatenate([piece, jnp.zeros((width - piece.shape[0], piece.shape[1]), piece.dtype)], axis=0)


def row_weight(hit, weight):
    return jnp.sum(jnp.where(hit, weight, 0.0), axis=1, keepdims=True)


def blocks(total, size):
    return [(start, min(size, total - start)) for start in range(0, total, size)]


def parts(rows):
    return rows * 3 // 5


def tiles(width):
    return -(-width // LANES)


def from_tiles(ref, first, count):
    peers = ref.shape[0]
    return jnp.concatenate([ref[:, first + i].reshape(peers * 8, LANES) for i in range(count)], axis=1)


def to_tiles(ref, first, value):
    rows, width = value.shape
    for i in range(tiles(width)):
        part = value[:, i * LANES : min(width, (i + 1) * LANES)]
        ref[:, first + i, :, pl.ds(0, part.shape[1])] = part.reshape(rows // 8, 8, part.shape[1]).astype(BF)


def pack_x_body(ids_ref, w_ref, x_ref, out_o, rank_ref, meta_ref, out_s, sems):
    rows, tokens = rank_ref.shape
    rank, _ = rank_rows(ids_ref[...], [], 0, rows // 8)
    rank_ref[...] = rank
    meta_ref[...] = jnp.concatenate([ids_ref[...].astype(F32), w_ref[...]], axis=0)
    slot = iota((rows, tokens), 0) % 8
    width = x_ref.shape[0]
    pieces = blocks(width, QW)
    spans = [(start // LANES, tiles(size)) for start, size in pieces] + [(tiles(width), tiles(QW))]
    copies = [
        pltpu.make_async_copy(out_s.at[:, pl.ds(c, n)], out_o.at[:, pl.ds(c, n)], sems.at[g])
        for g, (c, n) in enumerate(spans)
    ]
    main = onehot(rank == (slot + 1).astype(F32))
    for q, (start, size) in enumerate(pieces):
        to_tiles(out_s, spans[q][0], dot_nt(main, padded(x_ref[pl.ds(start, size), :], spans[q][1] * LANES)))
        copies[q].start()
    hit = rank == (slot % 2 + 9).astype(F32)
    picks = jnp.concatenate([onehot(hit & (slot // 2 == q)) for q in range(4)], axis=1)
    source = jnp.concatenate([padded(x_ref[pl.ds(start, size), :], QW) for start, size in pieces], axis=1)
    to_tiles(out_s, spans[4][0], dot_nt(picks, source))
    copies[4].start()
    for copy in copies:
        copy.wait()


def pack_x(ids, weights, x, peers):
    tokens = ids.shape[1]
    count = tiles(x.shape[0]) + tiles(QW)
    vmem = pl.BlockSpec(memory_space=pltpu.VMEM)
    return pl.pallas_call(
        pack_x_body,
        in_specs=[vmem, vmem, vmem],
        out_specs=[ANY, vmem, vmem],
        out_shape=[
            jax.ShapeDtypeStruct((peers, count, 8, LANES), BF),
            jax.ShapeDtypeStruct((peers * 8, tokens), F32),
            jax.ShapeDtypeStruct((2 * ids.shape[0], tokens), F32),
        ],
        scratch_shapes=[pltpu.VMEM((peers, count, 8, LANES), BF), pltpu.SemaphoreType.DMA((5,))],
        compiler_params=pltpu.CompilerParams(vmem_limit_bytes=VLIMIT),
        name="pack_x",
    )(ids, weights, x)


def pack_dy_body(zl_ref, pa_ref, pb_ref, ma_ref, mb_ref, out_o, pay, meta, ranks, scales, out_s, sems, isems):
    _, width, tokens = pay.shape
    peers = out_s.shape[0]
    rows = peers * 8
    top = meta.shape[1] // 2
    loads = [
        pltpu.make_async_copy(src, dst.at[i % 2], isems.at[i])
        for i, (src, dst) in enumerate(((ma_ref, meta), (mb_ref, meta), (pa_ref, pay), (pb_ref, pay)))
    ]
    for copy in loads:
        copy.start()
    for copy in loads:
        copy.wait()
    slot = iota((rows, tokens), 0) % 8
    spans = blocks(width, LW)

    def send(i, first, count):
        part = pl.ds(first, count)
        return pltpu.make_async_copy(out_s.at[:, part], out_o.at[:, part], sems.at[i])

    def source(s, carry):
        ids = meta[s, pl.ds(0, top), :].astype(jnp.int32)
        weight = meta[s, pl.ds(top, top), :]
        w1 = weight.astype(BF)
        rest = weight - w1.astype(F32)
        w2 = rest.astype(BF)
        w3 = (rest - w2.astype(F32)).astype(BF)
        rank, weight = rank_rows(ids, [w.astype(F32) for w in (w1, w2, w3)], zl_ref[0] * peers, peers)
        ranks[s] = rank
        scales[s] = weight
        hit = rank == (slot + 1).astype(F32)
        scale = row_weight(hit, weight)
        for i, (start, size) in enumerate(spans):
            count = tiles(size)
            first = 2 * (start // LANES) + s * count
            to_tiles(out_s, first, dot_nt(onehot(hit), padded(pay[s, pl.ds(start, size), :], count * LANES)) * scale)
            send(2 * s + i, first, count).start()
        return carry

    lax.fori_loop(0, 2, source, 0)
    picks, pieces = [], []
    scale = jnp.zeros((rows, 1), F32)
    for s in range(2):
        hit = ranks[s] == (slot % 2 + 9).astype(F32)
        scale = scale + jnp.where((slot[:, :1] // 2) % 2 == s, row_weight(hit, scales[s]), 0.0)
        for c, (start, size) in enumerate(spans):
            picks.append(onehot(hit & (slot // 2 == c * 2 + s)))
            pieces.append(padded(pay[s, pl.ds(start, size), :], LW))
    last = 2 * tiles(width)
    to_tiles(out_s, last, dot_nt(jnp.concatenate(picks, axis=1), jnp.concatenate(pieces, axis=1)) * scale)
    send(4, last, tiles(LW)).start()
    for s in range(2):
        for i, (start, size) in enumerate(spans):
            send(2 * s + i, 2 * (start // LANES) + s * tiles(size), tiles(size)).wait()
    send(4, last, tiles(LW)).wait()


def pack_dy(zl, dy_a, dy_b, meta_a, meta_b, peers):
    width, tokens = dy_a.shape
    shape = (peers, 2 * tiles(width) + tiles(LW), 8, LANES)
    return pl.pallas_call(
        pack_dy_body,
        in_specs=[SMEM, ANY, ANY, ANY, ANY],
        out_specs=ANY,
        out_shape=jax.ShapeDtypeStruct(shape, BF),
        scratch_shapes=[
            pltpu.VMEM((2,) + dy_a.shape, BF),
            pltpu.VMEM((2,) + meta_a.shape, F32),
            pltpu.VMEM((2, peers * 8, tokens), F32),
            pltpu.VMEM((2, peers * 8, tokens), F32),
            pltpu.VMEM(shape, BF),
            pltpu.SemaphoreType.DMA((5,)),
            pltpu.SemaphoreType.DMA((4,)),
        ],
        compiler_params=pltpu.CompilerParams(vmem_limit_bytes=VLIMIT),
    )(zl, dy_a, dy_b, meta_a, meta_b)


def load_plane(zl, slab, main, rem, sems):
    plane = slab.shape[0]
    count = main.shape[1]
    left = tiles(LW)
    right = count - left
    copies = []
    for z in range(2):
        rel = lax.bitwise_xor(zl, z)
        span = pl.ds(z * plane, plane)
        for i, (first, n) in enumerate(((rel * left, left), (2 * left + rel * right, right))):
            copies.append(
                pltpu.make_async_copy(
                    slab.at[:, pl.ds(first, n)], main.at[span, pl.ds(i * left, n)], sems.at[2 * z + i]
                )
            )
    copies.append(pltpu.make_async_copy(slab.at[:, pl.ds(2 * count, left)], rem, sems.at[4]))
    for copy in copies:
        copy.start()
    return copies


def place_main(main, dst):
    peers = main.shape[0]
    width = dst.shape[2]
    for c, (start, size) in enumerate(blocks(width, LANES)):
        dst[pl.ds(0, peers), :, pl.ds(start, size)] = main[:, c, :, pl.ds(0, size)]


def place_rem(zl, rem, dst):
    plane = rem.shape[0]
    peers = plane * 2
    last = from_tiles(rem, 0, rem.shape[1])
    r_i = iota((peers * 2, plane * 8), 0)
    c_i = iota((peers * 2, plane * 8), 1)
    rel = lax.bitwise_xor(r_i // peers, zl)
    base = ((r_i // 2) % plane) * 8 + rel * 2 + r_i % 2
    for c, (start, size) in enumerate(blocks(dst.shape[2], LW)):
        value = dot_nn(onehot(c_i == base + 4 * c), last[:, :size])
        dst[pl.ds(peers, peers // 4), :, pl.ds(start, size)] = value.reshape(peers // 4, 8, size).astype(BF)


def split_body(dp_ref, slab, x_o, xh_o, xs_o, got, x3, xh_s, xs_s, sems, osems):
    peers = slab.shape[0]
    main = peers * 8
    width = x3.shape[2]
    copy = pltpu.make_async_copy(slab, got, sems.at[0])
    copy.start()
    copy.wait()
    place_main(got, x3)
    last = from_tiles(got, tiles(width), tiles(QW))
    r_i = iota((peers * 2, main), 0)
    c_i = iota((peers * 2, main), 1)
    for q, (start, size) in enumerate(blocks(width, QW)):
        pick = onehot(c_i == (r_i // 2) * 8 + 2 * q + r_i % 2)
        value = dot_nn(pick, last[:, :size])
        x3[pl.ds(peers, peers // 4), :, pl.ds(start, size)] = value.reshape(peers // 4, 8, size).astype(BF)
    first = dp_ref[0] == 0
    x0 = x3[:, :, pl.ds(0, width // 2)]
    x1 = x3[:, :, pl.ds(width // 2, width // 2)]
    send = jnp.where(first, x1, x0)
    xs_s[...] = send.reshape(main + peers * 2, width // 2).T
    outs = [pltpu.make_async_copy(xs_s, xs_o, osems.at[0])]
    outs[0].start()
    outs.append(pltpu.make_async_copy(x3, x_o, osems.at[1]))
    outs[1].start()
    xh_s[...] = jnp.where(first, x0, x1)
    outs.append(pltpu.make_async_copy(xh_s, xh_o, osems.at[2]))
    outs[2].start()
    for copy in outs:
        copy.wait()


def split_x(dp, slab, width):
    peers = slab.shape[0]
    groups = peers * 10 // 8
    sds = jax.ShapeDtypeStruct
    half = (groups, 8, width // 2)
    return pl.pallas_call(
        split_body,
        in_specs=[SMEM, ANY],
        out_specs=[ANY] * 3,
        out_shape=[sds((groups, 8, width), BF), sds(half, BF), sds((width // 2, groups * 8), BF)],
        scratch_shapes=[
            pltpu.VMEM(slab.shape, BF),
            pltpu.VMEM((groups, 8, width), BF),
            pltpu.VMEM(half, BF),
            pltpu.VMEM((width // 2, groups * 8), BF),
            pltpu.SemaphoreType.DMA((1,)),
            pltpu.SemaphoreType.DMA((3,)),
        ],
        compiler_params=pltpu.CompilerParams(vmem_limit_bytes=VLIMIT),
        name="split_x",
    )(dp, slab)


def pre_body(x, wup, act_o, slope_o, x3, wu, act_s, slope_s, sems, osems):
    groups, _, width = x.shape
    rows = groups * 8
    hidden = wup.shape[0]
    copies = [pltpu.make_async_copy(x, x3, sems.at[0]), pltpu.make_async_copy(wup, wu, sems.at[1])]
    for copy in copies:
        copy.start()
    for copy in copies:
        copy.wait()

    def block(n, carry):
        span = pl.ds(pl.multiple_of(n * HB, HB), HB)
        pre = dot_nt(x3[...].reshape(rows, width), wu[span, :])
        s = jax.nn.sigmoid(pre)
        act_s[span, :] = (pre * s).T.astype(BF)
        slope_s[n] = s * (1.0 + pre * (1.0 - s))
        return carry

    lax.fori_loop(0, hidden // HB, block, 0)
    outs = [
        pltpu.make_async_copy(act_s, act_o, osems.at[0]),
        pltpu.make_async_copy(slope_s, slope_o, osems.at[1]),
    ]
    for copy in outs:
        copy.start()
    for copy in outs:
        copy.wait()


def expert_pre(x, wup):
    groups, _, width = x.shape
    rows = groups * 8
    hidden = wup.shape[0]
    sds = jax.ShapeDtypeStruct
    return pl.pallas_call(
        pre_body,
        in_specs=[ANY, ANY],
        out_specs=[ANY] * 2,
        out_shape=[sds((hidden, rows), BF), sds((hidden // HB, rows, HB), F32)],
        scratch_shapes=[
            pltpu.VMEM((groups, 8, width), BF),
            pltpu.VMEM((hidden, width), BF),
            pltpu.VMEM((hidden, rows), BF),
            pltpu.VMEM((hidden // HB, rows, HB), F32),
            pltpu.SemaphoreType.DMA((2,)),
            pltpu.SemaphoreType.DMA((2,)),
        ],
        compiler_params=pltpu.CompilerParams(vmem_limit_bytes=VLIMIT),
        cost_estimate=pl.CostEstimate(flops=2 * rows * hidden * width, transcendentals=rows * hidden, bytes_accessed=20_000_000),
        name="expert_pre",
    )(x, wup)


def grad_body(zl_ref, slab, slope, wup, wdn, ret_o, gp_o, gpa_o, gpb_o, dy_o, got, rem, dy3, wu, wd, slope_s, gp_n, gp_s, gpt_s, ret, rest, sems, osems):
    plane = slab.shape[0]
    peers = plane * 2
    main = peers * 8
    rows = main + peers * 2
    hidden, width = wu.shape
    zl = zl_ref[0]
    copies = load_plane(zl, slab, got, rem, sems)
    more = [
        pltpu.make_async_copy(src, dst, sems.at[5 + i])
        for i, (src, dst) in enumerate(((wdn, wd), (slope, slope_s), (wup, wu)))
    ]
    for copy in more:
        copy.start()
    for copy in copies:
        copy.wait()
    place_main(got, dy3)
    place_rem(zl, rem, dy3)
    outs = [pltpu.make_async_copy(dy3, dy_o, osems.at[0])]
    outs[0].start()
    for copy in more[:2]:
        copy.wait()

    def block(n, carry):
        span = pl.ds(pl.multiple_of(n * HB, HB), HB)
        grad = dot_nt(dy3[...].reshape(rows, width), wd[span, :])
        value = (grad * slope_s[n]).astype(BF)
        gp_n[n] = value
        gpt_s[span, :] = value.T
        return carry

    lax.fori_loop(0, hidden // HB, block, 0)
    for n in range(hidden // HB):
        gp_s[:, pl.ds(n * HB, HB)] = gp_n[n]
    cut = gpa_o.shape[1]
    for i, (src, dst) in enumerate(
        (
            (gpt_s.at[:, pl.ds(0, cut)], gpa_o),
            (gpt_s.at[:, pl.ds(cut, rows - cut)], gpb_o),
            (gpt_s, gp_o),
        )
    ):
        outs.append(pltpu.make_async_copy(src, dst, osems.at[7 + i]))
        outs[-1].start()
    more[2].wait()
    rest[...] = jnp.zeros(rest.shape, F32)
    r_j = iota((main, peers * 2), 0)
    c_j = iota((main, peers * 2), 1)

    def columns(q, start, size):
        value = dot_nn(gp_s[...], wu[:, pl.ds(start, size)]).astype(BF)
        to_tiles(ret, q * tiles(QW), value[:main])
        place = onehot(((r_j % 8) // 2 == q) & (c_j == (r_j // 8) * 2 + r_j % 2))
        rest[:, pl.ds(0, size)] = rest[:, pl.ds(0, size)] + dot_nn(place, value[main:])

    def send(q, first, count):
        part = pl.ds(first, count)
        return pltpu.make_async_copy(ret.at[:, part], ret_o.at[:, part], osems.at[2 + q])

    def step(q, carry):
        columns(q, pl.multiple_of(q * QW, QW), QW)
        send(q, q * tiles(QW), tiles(QW)).start()
        return carry

    full = width // QW
    end = width - full * QW
    ret[:, tiles(width) - 1] = jnp.zeros((peers, 8, LANES), BF)
    lax.fori_loop(0, full, step, 0)
    columns(full, full * QW, end)
    send(full, full * tiles(QW), tiles(end)).start()
    to_tiles(ret, tiles(width), rest[...])
    send(full + 1, tiles(width), tiles(QW)).start()
    outs += [send(q, q * tiles(QW), tiles(QW)) for q in range(full)]
    outs += [send(full, full * tiles(QW), tiles(end)), send(full + 1, tiles(width), tiles(QW))]
    for copy in outs:
        copy.wait()


def expert_grad(zl, slab, slope, wup, wdn):
    plane = slab.shape[0]
    peers = plane * 2
    hidden, width = wup.shape
    rows = peers * 10
    groups = rows // 8
    cut = parts(rows)
    count = tiles(width) + tiles(QW)
    sds = jax.ShapeDtypeStruct
    return pl.pallas_call(
        grad_body,
        in_specs=[SMEM, ANY, ANY, ANY, ANY],
        out_specs=[ANY] * 5,
        out_shape=[sds((peers, count, 8, LANES), BF), sds((hidden, rows), BF)] + [sds((hidden, n), BF) for n in (cut, rows - cut)] + [sds((groups, 8, width), BF)],
        scratch_shapes=[
            pltpu.VMEM((peers, tiles(width), 8, LANES), BF),
            pltpu.VMEM((plane, tiles(LW), 8, LANES), BF),
            pltpu.VMEM((groups, 8, width), BF),
            pltpu.VMEM((hidden, width), BF),
            pltpu.VMEM((hidden, width), BF),
            pltpu.VMEM(slope.shape, F32),
            pltpu.VMEM(slope.shape, BF),
            pltpu.VMEM((rows, hidden), BF),
            pltpu.VMEM((hidden, rows), BF),
            pltpu.VMEM((peers, count, 8, LANES), BF),
            pltpu.VMEM((peers * 8, QW), F32),
            pltpu.SemaphoreType.DMA((8,)),
            pltpu.SemaphoreType.DMA((10,)),
        ],
        compiler_params=pltpu.CompilerParams(vmem_limit_bytes=VLIMIT),
        cost_estimate=pl.CostEstimate(flops=4 * rows * hidden * width, transcendentals=0, bytes_accessed=40_000_000),
        name="expert_grad",
    )(zl, slab, slope, wup, wdn)


def unpack_body(zl_ref, slab, dy_o, got, rem, dy3, sems):
    for copy in load_plane(zl_ref[0], slab, got, rem, sems):
        copy.wait()
    place_main(got, dy3)
    place_rem(zl_ref[0], rem, dy3)
    copy = pltpu.make_async_copy(dy3, dy_o, sems.at[5])
    copy.start()
    copy.wait()


def unpack_other(zl, slab, width):
    plane = slab.shape[0]
    peers = plane * 2
    groups = peers * 10 // 8
    return pl.pallas_call(
        unpack_body,
        in_specs=[SMEM, ANY],
        out_specs=ANY,
        out_shape=jax.ShapeDtypeStruct((groups, 8, width), BF),
        scratch_shapes=[
            pltpu.VMEM((peers, tiles(width), 8, LANES), BF),
            pltpu.VMEM((plane, tiles(LW), 8, LANES), BF),
            pltpu.VMEM((groups, 8, width), BF),
            pltpu.SemaphoreType.DMA((6,)),
        ],
        compiler_params=pltpu.CompilerParams(vmem_limit_bytes=VLIMIT),
        name="unpack_other",
    )(zl, slab)


def combine_body(rank_ref, ret_ref, out_o, got, out_ref, sems, osems):
    rows, tokens = rank_ref.shape
    width = out_ref.shape[0]
    outs = []
    spans = [(tiles(width), tiles(QW))] + [(start // LANES, tiles(size)) for start, size in blocks(width, QW)]
    copies = [
        pltpu.make_async_copy(ret_ref.at[:, pl.ds(c, n)], got.at[:, pl.ds(c, n)], sems.at[i])
        for i, (c, n) in enumerate(spans)
    ]
    for copy in copies:
        copy.start()
    slot = iota((rows, tokens), 0) % 8
    rank = rank_ref[...]
    last = rank == (slot % 2 + 9).astype(F32)
    picks = jnp.concatenate([onehot(last & (slot // 2 == q)) for q in range(4)], axis=1)
    main = onehot(rank == (slot + 1).astype(F32))
    copies[0].wait()
    rem = dot_tn(picks, from_tiles(got, *spans[0]))
    for q, (start, size) in enumerate(blocks(width, QW)):
        copies[1 + q].wait()
        value = dot_tn(main, from_tiles(got, *spans[1 + q]))[:, :size]
        value = value + rem[q * tokens : (q + 1) * tokens, :size]
        out_ref[pl.ds(start, size), :] = value.T.astype(BF)
        outs.append(pltpu.make_async_copy(out_ref.at[pl.ds(start, size)], out_o.at[pl.ds(start, size)], osems.at[q]))
        outs[-1].start()
    for copy in outs:
        copy.wait()


def combine(rank, ret, width):
    vmem = pl.BlockSpec(memory_space=pltpu.VMEM)
    return pl.pallas_call(
        combine_body,
        in_specs=[vmem, ANY],
        out_specs=ANY,
        out_shape=jax.ShapeDtypeStruct((width, rank.shape[1]), BF),
        scratch_shapes=[
            pltpu.VMEM(ret.shape, BF),
            pltpu.VMEM((width, rank.shape[1]), BF),
            pltpu.SemaphoreType.DMA((5,)),
            pltpu.SemaphoreType.DMA((4,)),
        ],
        compiler_params=pltpu.CompilerParams(vmem_limit_bytes=VLIMIT),
        name="combine",
    )(rank, ret)


def local(sizes, tokens_in, grad_out, expert_ids, combine_weights, up_weight, down_weight):
    n_dp, n_zl, n_plane = sizes
    peers = n_zl * n_plane
    width = tokens_in.shape[1]
    x = tokens_in.T
    dy = grad_out.T
    ids = expert_ids.T
    weights = combine_weights.T
    wup = up_weight[0].T
    wdn = down_weight[0]
    dp = lax.axis_index("dp").astype(jnp.int32)
    zl = lax.axis_index("zl").astype(jnp.int32)

    def move(value, cross, flip):
        pairs = []
        for i in range(n_dp * peers):
            d, z, p = i // peers, (i // n_plane) % n_zl, i % n_plane
            pairs.append((i, ((d ^ cross) * n_zl + (z ^ flip)) * n_plane + p))
        return lax.ppermute(value, ALL, pairs)

    slab, rank, meta = pack_x(ids, weights, x, peers)
    dy_near = move(dy, 0, 1)
    meta_near = move(meta, 0, 1)
    dy_a, meta_a = move(dy, 1, 0), move(meta, 1, 0)
    dy_b, meta_b = move(dy, 1, 1), move(meta, 1, 1)

    got_x = lax.all_to_all(slab, GROUP, 0, 0, tiled=True)
    slab_dy = pack_dy(zl[None], dy, dy_near, meta, meta_near, n_plane)
    got_dy = lax.all_to_all(slab_dy, PLANE, 0, 0, tiled=True)
    slab_other = pack_dy(zl[None], dy_a, dy_b, meta_a, meta_b, n_plane)
    got_other = lax.all_to_all(slab_other, PLANE, 0, 0, tiled=True)

    x_rows, xh, x_send = split_x(dp[None], got_x, width)
    act, slope = expert_pre(x_rows, wup)
    xh_other = move(x_send, 1, 0)
    act_keep = lax.dynamic_slice_in_dim(act, dp * (act.shape[0] // 2), act.shape[0] // 2, 0)
    act_send = lax.dynamic_slice_in_dim(act, (1 - dp) * (act.shape[0] // 2), act.shape[0] // 2, 0)
    act_other = move(act_send, 1, 0)
    ret, gp, gpa, gpb, dyr = expert_grad(zl[None], got_dy, slope, wup, wdn)
    gpa_other = move(gpa, 1, 0)
    gpb_other = move(gpb, 1, 0)
    back = lax.all_to_all(ret, GROUP, 0, 0, tiled=True)
    dy_other = unpack_other(zl[None], got_other, width)

    flat = lambda a: a.reshape(-1, a.shape[-1])
    up = lambda a, b: lax.dot_general(a, b, (((0,), (1,)), ((), ())), preferred_element_type=F32)
    grad_down = (dot_nn(act_keep, flat(dyr)) + dot_nn(act_other, flat(dy_other))).astype(BF)[None]
    cut = gpa.shape[1]
    early = dot_nt(xh_other[:, :cut], gpa_other) + up(flat(xh), gp)
    grad_up = (dot_nt(xh_other[:, cut:], gpb_other) + early).astype(BF)[None]
    grad_input = combine(rank, back, width).T
    return grad_input, grad_up, grad_down


def build(devices, shape):
    n_dp, n_zl, n_y, n_x, n_core = shape
    fine = Mesh(devices.reshape(shape), ALL)
    token = P(ALL, None)
    weight = P(GROUP, None, None)
    inner = functools.partial(local, (n_dp, n_zl, n_y * n_x * n_core))

    return jax.shard_map(
        inner,
        mesh=fine,
        in_specs=(token, token, token, token, weight, weight),
        out_specs=(token, P(GROUP, "dp", None), P(GROUP, "dp", None)),
        check_vma=False,
    )


def solution(mesh):
    return build(mesh.devices, (2, 2, 4, 4, 2))
```
